8 devices in a mesh: data: 2 (over z, y), stage: 4 (over x, core).
Axes of the slice: x: 2, y: 2, z: 1, core: 2. Of those that a mesh axis runs over, the one named last changes fastest.
Arguments:
- x_enc: bfloat16 [256, 128, 1024], P(('data', 'stage')), parts along dimension 0
- enc_len: int32 [256], P(('data', 'stage')), parts along dimension 0
- y: bfloat16 [256, 48, 1024], P(('data', 'stage')), parts along dimension 0
- enc_wqkv: bfloat16 [2, 1024, 3, 16, 128], replicated
- enc_wo: bfloat16 [2, 16, 128, 1024], replicated
- enc_w1: bfloat16 [2, 1024, 3072], replicated
- enc_w2: bfloat16 [2, 3072, 1024], replicated
- dec_wqkv: bfloat16 [2, 1024, 3, 16, 128], replicated
- dec_wo: bfloat16 [2, 16, 128, 1024], replicated
- cross_wq: bfloat16 [2, 1024, 8, 2, 128], replicated
- cross_wkv: bfloat16 [2, 1024, 2, 8, 128], replicated
- cross_wo: bfloat16 [2, 8, 2, 128, 1024], replicated
- dec_w1: bfloat16 [2, 1024, 3072], replicated
- dec_w2: bfloat16 [2, 3072, 1024], replicated
Outputs:
- output: bfloat16 [256, 48, 1024], P(('data', 'stage')), parts along dimension 0
There are 2 independent parts. The reference program is written for one: setup_inputs(seed, part) draws one part's arguments, and reference() takes and returns one part's arrays. A program takes and returns all parts, laid end to end along the dimension named above; an argument that names none is the same for every part.
All inputs are finite; a program needn't handle non-finite values.
Results may differ from the reference program's by a relative error of at most 0.0125606.
Values are sent between devices in bfloat16 or wider.
A program may use at most 1 GiB of HBM per device.

```python
import jax
import jax.numpy as jnp
from jax import lax

D = 1024
HEADS = 16
KV_HEADS = 8
HEAD = 128
FF = 3072
S_ENC = 128
S_DEC = 48
N_SEQ = 128
L_ENC = 2
L_DEC = 2

REP = HEADS // KV_HEADS


def weight(weight_key, shape, fan_in):
    return (jax.random.normal(weight_key, shape, jnp.float32) * fan_in ** -0.5).astype(jnp.bfloat16)


def structured(key_set, length):
    trend = jnp.linspace(-1.0, 1.0, length)[None, :, None]
    common = jax.random.normal(key_set[0], (N_SEQ, 1, D), jnp.float32)
    slope = jax.random.normal(key_set[1], (N_SEQ, 1, D), jnp.float32)
    noise = jax.random.normal(key_set[2], (N_SEQ, length, D), jnp.float32)
    return (0.5 * common + 0.8 * trend * slope + 0.4 * noise).astype(jnp.bfloat16)


def setup_inputs(seed: int = 0, part: int = 0) -> dict:
    part_keys = jax.random.split(jax.random.fold_in(jax.random.key(seed), part), 7)
    weight_keys = jax.random.split(jax.random.key(seed + 1), 11)
    lengths = jax.random.randint(part_keys[6], (N_SEQ,), S_ENC // 4, S_ENC + 1, jnp.int32)
    lengths = lengths.at[0].set(S_ENC)
    return {
        "x_enc": structured(part_keys[0:3], S_ENC),
        "enc_len": lengths,
        "y": structured(part_keys[3:6], S_DEC),
        "enc_wqkv": weight(weight_keys[0], (L_ENC, D, 3, HEADS, HEAD), D),
        "enc_wo": weight(weight_keys[1], (L_ENC, HEADS, HEAD, D), HEADS * HEAD),
        "enc_w1": weight(weight_keys[2], (L_ENC, D, FF), D),
        "enc_w2": weight(weight_keys[3], (L_ENC, FF, D), FF),
        "dec_wqkv": weight(weight_keys[4], (L_DEC, D, 3, HEADS, HEAD), D),
        "dec_wo": weight(weight_keys[5], (L_DEC, HEADS, HEAD, D), HEADS * HEAD),
        "cross_wq": weight(weight_keys[6], (L_DEC, D, KV_HEADS, REP, HEAD), D),
        "cross_wkv": weight(weight_keys[7], (L_DEC, D, 2, KV_HEADS, HEAD), D),
        "cross_wo": weight(weight_keys[8], (L_DEC, KV_HEADS, REP, HEAD, D), HEADS * HEAD),
        "dec_w1": weight(weight_keys[9], (L_DEC, D, FF), D),
        "dec_w2": weight(weight_keys[10], (L_DEC, FF, D), FF),
    }


def rms_norm(inputs):
    wide = inputs.astype(jnp.float32)
    return (wide * lax.rsqrt(jnp.mean(wide * wide, axis=-1, keepdims=True) + 1e-6)).astype(jnp.bfloat16)


def attend(query, keys, values, valid):
    scores = jnp.einsum("qgrd,kgd->grqk", query.astype(jnp.float32), keys.astype(jnp.float32)) * HEAD ** -0.5
    attn_probs = jax.nn.softmax(jnp.where(valid, scores, -1e30), axis=-1).astype(jnp.bfloat16)
    return jnp.einsum("grqk,kgd->qgrd", attn_probs.astype(jnp.float32), values.astype(jnp.float32)).astype(jnp.bfloat16)


def self_block(state, w_qkv, w_out, valid):
    proj_qkv = jnp.einsum("sd,dthe->tshe", rms_norm(state).astype(jnp.float32), w_qkv.astype(jnp.float32)).astype(jnp.bfloat16)
    mixed = attend(proj_qkv[0][:, :, None, :], proj_qkv[1], proj_qkv[2], valid)
    update = jnp.einsum("shre,hev->sv", mixed.astype(jnp.float32), w_out.astype(jnp.float32))
    return (state.astype(jnp.float32) + update).astype(jnp.bfloat16)


def ffn_block(state, w_in, w_out):
    hidden = jax.nn.gelu(jnp.dot(rms_norm(state), w_in, preferred_element_type=jnp.float32)).astype(jnp.bfloat16)
    return (state.astype(jnp.float32) + jnp.dot(hidden, w_out, preferred_element_type=jnp.float32)).astype(jnp.bfloat16)


def reference(x_enc, enc_len, y, enc_wqkv, enc_wo, enc_w1, enc_w2, dec_wqkv, dec_wo, cross_wq, cross_wkv, cross_wo, dec_w1, dec_w2):
    def encode_one(pair):
        state = pair[0]
        valid = jnp.arange(S_ENC) < pair[1]
        for layer in range(L_ENC):
            state = self_block(state, enc_wqkv[layer], enc_wo[layer], valid)
            state = ffn_block(state, enc_w1[layer], enc_w2[layer])
        return rms_norm(state)

    enc_states = lax.map(encode_one, (x_enc, enc_len))
    partner_out = jnp.roll(enc_states, N_SEQ // 2, axis=0)
    partner_len = jnp.roll(enc_len, N_SEQ // 2, axis=0)
    positions = jnp.arange(S_DEC)
    causal = positions[None, :] <= positions[:, None]

    def decode_one(triple):
        state, enc_seq, length = triple
        keep = jnp.arange(S_ENC) < length
        for layer in range(L_DEC):
            state = self_block(state, dec_wqkv[layer], dec_wo[layer], causal)
            query = jnp.einsum("sd,dgre->sgre", rms_norm(state).astype(jnp.float32), cross_wq[layer].astype(jnp.float32)).astype(jnp.bfloat16)
            key_vals = jnp.einsum("sd,dtge->tsge", enc_seq.astype(jnp.float32), cross_wkv[layer].astype(jnp.float32)).astype(jnp.bfloat16)
            mixed = attend(query, key_vals[0], key_vals[1], keep)
            update = jnp.einsum("sgre,grev->sv", mixed.astype(jnp.float32), cross_wo[layer].astype(jnp.float32))
            state = (state.astype(jnp.float32) + update).astype(jnp.bfloat16)
            state = ffn_block(state, dec_w1[layer], dec_w2[layer])
        return state

    return lax.map(decode_one, (y, partner_out, partner_len))
```

```python
import jax
import jax.numpy as jnp
from jax import lax
from jax.experimental import pallas as pl
from jax.experimental.pallas import tpu as pltpu
from jax.sharding import PartitionSpec as P

BF = jnp.bfloat16
F32 = jnp.float32
D = 1024
HEADS = 16
HD = 128
FF = 3072
S_ENC = 128
S_DEC = 48
TILE = 256
DTILE = 192
GROUP = 4
LOG2E = 1.4426950408889634
SCALE2 = HD ** -0.5 * LOG2E
VMEM_LIMIT = 66_000_000


def rms(h):
    wide = h.astype(F32)
    return (wide * lax.rsqrt(jnp.mean(wide * wide, axis=-1, keepdims=True) + 1e-6)).astype(BF)


def mm(lhs, rhs):
    return jnp.dot(lhs, rhs, preferred_element_type=F32)


def gelu(v):
    return jax.nn.gelu(v, approximate=True)


def softmax(s):
    m = jnp.max(s, axis=-1, keepdims=True)
    e = jnp.exp2((s - m) * SCALE2)
    return (e * (1.0 / jnp.sum(e, axis=-1, keepdims=True))).astype(BF)


def qk(q, k):
    return lax.dot_general(q, k, (((1,), (1,)), ((), ())), preferred_element_type=F32)


def prefix_starts(len_ref, starts, n):
    def step(i, pos):
        starts[i] = pos
        return pos + ((len_ref[i] + 15) // 16) * 16
    return lax.fori_loop(0, n, step, jnp.int32(0))


def head_copies(hbm, buf, sem, layer, heads, first):
    return [pltpu.make_async_copy(hbm.at[layer, c], buf.at[:, c * HD:(c + 1) * HD], sem.at[first + c]) for c in heads]


def start_all(copies):
    for c in copies:
        c.start()


def wait_all(copies):
    for c in copies:
        c.wait()


def enc_kernel(n_seq, len_ref, x_hbm, wqkv_hbm, wo_hbm, w1_hbm, w2_hbm, out_hbm,
               starts, h, qkv_a, qkv_b, o, s_scr, p_scr, xn, hid, wqkv, wo, w1, w2, sem_x, sem_w, sem_o):
    gw = GROUP * HD
    n_groups = HEADS // GROUP
    n_pair = n_seq // 2
    bufs = (qkv_a, qkv_b)

    def qkv_copies(layer, g):
        heads = [t * HEADS + g * GROUP + c for t in range(3) for c in range(GROUP)]
        return head_copies(wqkv_hbm, wqkv, sem_w, layer, heads, 0)

    def wo_copy(layer):
        return pltpu.make_async_copy(wo_hbm.at[layer], wo, sem_w.at[48])

    def w1_copy(layer):
        return pltpu.make_async_copy(w1_hbm.at[layer], w1, sem_w.at[49])

    def w2_copy(layer):
        return pltpu.make_async_copy(w2_hbm.at[layer], w2, sem_w.at[50])

    total = prefix_starts(len_ref, starts, n_seq)
    nt = (total + TILE - 1) // TILE
    end = pl.multiple_of(nt * TILE, TILE)
    last = pl.multiple_of((nt - 1) * TILE, TILE)
    h[pl.ds(last, TILE), :] = jnp.zeros((TILE, D), BF)

    def x_copy(s, j):
        src = x_hbm.at[pl.ds(pl.multiple_of(s * S_ENC + j * 16, 16), 16), :]
        dst = h.at[pl.ds(pl.multiple_of(starts[s] + j * 16, 16), 16), :]
        return pltpu.make_async_copy(src, dst, sem_x)

    def each_piece(fn):
        def seq(s, c):
            lax.fori_loop(0, (len_ref[s] + 15) // 16, lambda j, d: (fn(s, j), d)[1], 0)
            return c
        lax.fori_loop(0, n_seq, seq, 0)

    each_piece(lambda s, j: x_copy(s, j).start())
    for g in range(n_groups):
        start_all(qkv_copies(0, g))
    wo_copy(0).start()
    w1_copy(0).start()
    w2_copy(0).start()
    o[pl.ds(last, TILE), :] = jnp.zeros((TILE, HEADS * HD), BF)
    for buf in bufs:
        buf[pl.ds(end, S_ENC), :] = jnp.zeros((S_ENC, 3 * gw), BF)
    each_piece(lambda s, j: x_copy(s, j).wait())

    def layer_step(layer, carry):
        def project_part(i, g, t):
            r = pl.ds(pl.multiple_of(i * TILE, TILE), TILE)
            c0 = (t * HEADS + g * GROUP) * HD
            bufs[g % 2][r, t * gw:(t + 1) * gw] = mm(xn[...], wqkv[:, c0:c0 + gw]).astype(BF)

        def norm(i):
            xn[...] = rms(h[pl.ds(pl.multiple_of(i * TILE, TILE), TILE), :])

        def rows_of(s):
            return pl.ds(pl.multiple_of(starts[s], 16), S_ENC)

        def scores(pi, g):
            buf = bufs[g % 2]
            for b in range(2):
                s = 2 * pi + b
                r = rows_of(s)
                keep = lax.broadcasted_iota(jnp.int32, (S_ENC, S_ENC), 1) < len_ref[s]
                for hh in range(GROUP):
                    c = hh * HD
                    s_scr[b * GROUP + hh] = jnp.where(keep, qk(buf[r, c:c + HD], buf[r, gw + c:gw + c + HD]), -1e30)

        def probs():
            for j in range(2 * GROUP):
                p_scr[j] = softmax(s_scr[j])

        def values(pi, g):
            buf = bufs[g % 2]
            for b in range(2):
                r = rows_of(2 * pi + b)
                for hh in range(GROUP):
                    c = hh * HD
                    o[r, g * gw + c:g * gw + c + HD] = mm(p_scr[b * GROUP + hh], buf[r, 2 * gw + c:2 * gw + c + HD]).astype(BF)

        for g in range(n_groups + 1):
            if g < n_groups:
                wait_all(qkv_copies(layer, g))

            def project_only(i, c):
                norm(i)
                for t in range(3):
                    project_part(i, g, t)
                return c

            def both(i, c):
                scores(i, g - 1)
                norm(i)
                project_part(i, g, 0)
                probs()
                project_part(i, g, 1)
                project_part(i, g, 2)
                values(i, g - 1)
                return c

            def attend_only(i, c):
                scores(i, g - 1)
                probs()
                values(i, g - 1)
                return c

            if g == 0:
                lax.fori_loop(0, nt, project_only, 0)
            elif g < n_groups:
                lax.fori_loop(0, nt, both, 0)
                lax.fori_loop(nt, n_pair, attend_only, 0)
            else:
                lax.fori_loop(0, n_pair, attend_only, 0)

            if g < n_groups:
                @pl.when(layer == 0)
                def _():
                    start_all(qkv_copies(1, g))

        wo_copy(layer).wait()
        w1_copy(layer).wait()
        w2_copy(layer).wait()

        def ffn_tile(i, c):
            r = pl.ds(pl.multiple_of(i * TILE, TILE), TILE)
            for n in range(0, D, 512):
                h[r, n:n + 512] = (h[r, n:n + 512].astype(F32) + mm(o[r, :], wo[:, n:n + 512])).astype(BF)
            xn[...] = rms(h[r, :])
            for n in range(0, FF, 512):
                hid[:, n:n + 512] = gelu(mm(xn[...], w1[:, n:n + 512])).astype(BF)
            for n in range(0, D, 512):
                h[r, n:n + 512] = (h[r, n:n + 512].astype(F32) + mm(hid[...], w2[:, n:n + 512])).astype(BF)
            return c
        lax.fori_loop(0, nt, ffn_tile, 0)

        @pl.when(layer == 0)
        def _():
            wo_copy(1).start()
            w1_copy(1).start()
            w2_copy(1).start()
        return carry
    lax.fori_loop(0, 2, layer_step, 0)

    def out_copy(i):
        r = pl.ds(pl.multiple_of(i * TILE, TILE), TILE)
        return pltpu.make_async_copy(h.at[r, :], out_hbm.at[r, :], sem_o)

    def out_tile(i, c):
        r = pl.ds(pl.multiple_of(i * TILE, TILE), TILE)
        h[r, :] = rms(h[r, :])
        out_copy(i).start()
        return c
    lax.fori_loop(0, nt, out_tile, 0)
    lax.fori_loop(0, nt, lambda i, c: (out_copy(i).wait(), c)[1], 0)


ANY = pl.BlockSpec(memory_space=pl.ANY)
SMEM = pl.BlockSpec(memory_space=pltpu.SMEM)


def encode(lens, x, wqkv, wo, w1, w2):
    n_seq = lens.shape[0]
    rows = n_seq * S_ENC
    pad = rows + S_ENC
    tokens = rows * 5 // 8
    cost = pl.CostEstimate(flops=tokens * 2 * 30_400_000, bytes_accessed=70_000_000, transcendentals=0)
    return pl.pallas_call(
        lambda *refs: enc_kernel(n_seq, *refs),
        out_shape=jax.ShapeDtypeStruct((rows, D), BF),
        in_specs=[SMEM] + [ANY] * 5,
        out_specs=ANY,
        scratch_shapes=[
            pltpu.SMEM((n_seq,), jnp.int32),
            pltpu.VMEM((rows, D), BF),
            pltpu.VMEM((pad, 3 * GROUP * HD), BF),
            pltpu.VMEM((pad, 3 * GROUP * HD), BF),
            pltpu.VMEM((pad, 2 * D), BF),
            pltpu.VMEM((2 * GROUP, S_ENC, S_ENC), F32),
            pltpu.VMEM((2 * GROUP, S_ENC, S_ENC), BF),
            pltpu.VMEM((TILE, D), BF),
            pltpu.VMEM((TILE, FF), BF),
            pltpu.VMEM((D, 6 * D), BF),
            pltpu.VMEM((2 * D, D), BF),
            pltpu.VMEM((D, FF), BF),
            pltpu.VMEM((FF, D), BF),
            pltpu.SemaphoreType.DMA,
            pltpu.SemaphoreType.DMA((51,)),
            pltpu.SemaphoreType.DMA,
        ],
        compiler_params=pltpu.CompilerParams(vmem_limit_bytes=VMEM_LIMIT),
        cost_estimate=cost,
        name="encode",
    )(lens, x, wqkv, wo, w1, w2)


def dec_kernel(n_seq, len_ref, y_hbm, h1_hbm, h2_hbm, wqkv_hbm, wo_hbm, wq_hbm, wkv_hbm, woc_hbm, w1_hbm, w2_hbm, out_hbm,
               starts, z, kv, ht, qkv, o, s_scr, p_scr, xn, hid, wqkv, wo, wq, wkv, woc, w1, w2, sem_y, sem_w, sem_h):
    tokens = n_seq * S_DEC
    n_half = n_seq // 2
    wide = {0: (wqkv_hbm, wqkv, 48, 0), 2: (wkv_hbm, wkv, 16, 48), 3: (wq_hbm, wq, 16, 64)}
    flat = {1: (wo_hbm, wo, 80), 4: (woc_hbm, woc, 81), 5: (w1_hbm, w1, 82), 6: (w2_hbm, w2, 83)}

    class Copies:
        def __init__(self, copies):
            self.copies = copies

        def start(self):
            start_all(self.copies)

        def wait(self):
            wait_all(self.copies)

    def w_copy(layer, i):
        if i in wide:
            hbm, buf, n, first = wide[i]
            return Copies(head_copies(hbm, buf, sem_w, layer, range(n), first))
        hbm, buf, k = flat[i]
        return Copies([pltpu.make_async_copy(hbm.at[layer], buf, sem_w.at[k])])

    y_copy = pltpu.make_async_copy(y_hbm, z, sem_y)
    y_copy.start()
    for i in range(7):
        w_copy(0, i).start()

    def step(i, pos):
        pos = jnp.where(i == n_half, 0, pos)
        starts[i] = pos
        return pos + ((len_ref[i] + 15) // 16) * 16

    def total_of(lo):
        return lax.fori_loop(lo, lo + n_half, lambda i, t: t + ((len_ref[i] + 15) // 16) * 16, jnp.int32(0))
    lax.fori_loop(0, n_seq, step, jnp.int32(0))
    nts = [(total_of(hf * n_half) + TILE - 1) // TILE for hf in range(2)]
    y_copy.wait()

    pair = 2 * S_DEC
    qpos = lax.broadcasted_iota(jnp.int32, (pair, pair), 0)
    kpos = lax.broadcasted_iota(jnp.int32, (pair, pair), 1)
    causal = (kpos <= qpos) & ((kpos >= S_DEC) == (qpos >= S_DEC))

    def prefetch(layer, i):
        @pl.when(layer == 0)
        def _():
            w_copy(1, i).start()

    def layer_step(layer, carry):
        w_copy(layer, 0).wait()
        w_copy(layer, 1).wait()

        def self_tile(i, c):
            r = pl.ds(pl.multiple_of(i * DTILE, DTILE), DTILE)
            xn[:DTILE, :] = rms(z[r, :])
            gw = GROUP * HD
            n_groups = HEADS // GROUP
            n_pairs = DTILE // pair

            def project(g):
                for t in range(3):
                    c0 = t * 2 * D + g * gw
                    qkv[:, c0:c0 + gw] = mm(xn[:DTILE, :], wqkv[:, c0:c0 + gw]).astype(BF)

            def scores(g):
                for b in range(n_pairs):
                    rr = slice(b * pair, (b + 1) * pair)
                    for hh in range(GROUP):
                        c0 = g * gw + hh * HD
                        sc = qk(qkv[rr, c0:c0 + HD], qkv[rr, 2 * D + c0:2 * D + c0 + HD])
                        s_scr[(g % 2) * 16 + b * GROUP + hh, :, :pair] = jnp.where(causal, sc, -1e30)

            def values(g):
                for b in range(n_pairs):
                    rr = slice(b * pair, (b + 1) * pair)
                    for hh in range(GROUP):
                        c0 = g * gw + hh * HD
                        p = p_scr[(g % 2) * 16 + b * GROUP + hh, :, :pair]
                        o[rr, c0:c0 + HD] = mm(p, qkv[rr, 4 * D + c0:4 * D + c0 + HD]).astype(BF)

            def probs(g):
                for j in range(n_pairs * GROUP):
                    j = (g % 2) * 16 + j
                    p_scr[j, :, :pair] = softmax(s_scr[j, :, :pair])

            for g in range(n_groups + 1):
                if g < n_groups:
                    project(g)
                    scores(g)
                    probs(g)
                if g > 0:
                    values(g - 1)
            for n in range(0, D, 512):
                z[r, n:n + 512] = (z[r, n:n + 512].astype(F32) + mm(o[...], wo[:, n:n + 512])).astype(BF)
            return c
        lax.fori_loop(0, tokens // DTILE, self_tile, 0)
        prefetch(layer, 0)
        prefetch(layer, 1)

        w_copy(layer, 2).wait()
        w_copy(layer, 3).wait()
        w_copy(layer, 4).wait()
        for hf in range(2):
            nt = nts[hf]
            h_hbm = (h1_hbm, h2_hbm)[hf]

            def h_copy(i):
                src = h_hbm.at[pl.ds(pl.multiple_of(i * TILE, TILE), TILE), :]
                return pltpu.make_async_copy(src, ht.at[lax.rem(i, 2)], sem_h.at[lax.rem(i, 2)])
            h_copy(0).start()
            kv[pl.ds(pl.multiple_of(nt * TILE, TILE), S_ENC), :] = jnp.zeros((S_ENC, 2 * D), BF)

            def kv_tile(i, c):
                @pl.when(i + 1 < nt)
                def _():
                    h_copy(i + 1).start()
                h_copy(i).wait()
                r = pl.ds(pl.multiple_of(i * TILE, TILE), TILE)
                for n in range(0, 2 * D, D):
                    kv[r, n:n + D] = mm(ht[lax.rem(i, 2)], wkv[:, n:n + D]).astype(BF)
                return c
            lax.fori_loop(0, nt, kv_tile, 0)

            def cross_tile(i, c):
                base = hf * n_half
                r = pl.ds(pl.multiple_of(base * S_DEC + i * DTILE, DTILE), DTILE)
                xn[:DTILE, :] = rms(z[r, :])
                n_b = DTILE // S_DEC
                gw = 2 * GROUP * HD

                def project(g):
                    qkv[:, g * gw:(g + 1) * gw] = mm(xn[:DTILE, :], wq[:, g * gw:(g + 1) * gw]).astype(BF)

                def where_of(b):
                    s = base + i * n_b + b
                    return s, pl.ds(pl.multiple_of(starts[s], 16), S_ENC), slice(b * S_DEC, (b + 1) * S_DEC)

                def scores(g):
                    for b in range(n_b):
                        s, kr, rr = where_of(b)
                        keep = lax.broadcasted_iota(jnp.int32, (pair, S_ENC), 1) < len_ref[s]
                        for hh in range(GROUP):
                            c0 = g * gw + 2 * hh * HD
                            k0 = (g * GROUP + hh) * HD
                            q2 = jnp.concatenate([qkv[rr, c0:c0 + HD], qkv[rr, c0 + HD:c0 + 2 * HD]], axis=0)
                            s_scr[g * 16 + b * GROUP + hh] = jnp.where(keep, qk(q2, kv[kr, k0:k0 + HD]), -1e30)

                def probs(g):
                    for j in range(16):
                        p_scr[g * 16 + j] = softmax(s_scr[g * 16 + j])

                def values(g):
                    for b in range(n_b):
                        s, kr, rr = where_of(b)
                        for hh in range(GROUP):
                            c0 = g * gw + 2 * hh * HD
                            k0 = D + (g * GROUP + hh) * HD
                            res = mm(p_scr[g * 16 + b * GROUP + hh], kv[kr, k0:k0 + HD]).astype(BF)
                            o[rr, c0:c0 + HD] = res[:S_DEC]
                            o[rr, c0 + HD:c0 + 2 * HD] = res[S_DEC:]

                project(0)
                scores(0)
                probs(0)
                project(1)
                scores(1)
                probs(1)
                values(0)
                values(1)
                for n in range(0, D, 512):
                    z[r, n:n + 512] = (z[r, n:n + 512].astype(F32) + mm(o[...], woc[:, n:n + 512])).astype(BF)
                return c
            lax.fori_loop(0, n_half * S_DEC // DTILE, cross_tile, 0)
        prefetch(layer, 2)
        prefetch(layer, 3)
        prefetch(layer, 4)

        w_copy(layer, 5).wait()
        w_copy(layer, 6).wait()

        def ffn_tile(i, c):
            r = pl.ds(pl.multiple_of(i * TILE, TILE), TILE)
            xn[...] = rms(z[r, :])
            for n in range(0, FF, 512):
                hid[:, n:n + 512] = gelu(mm(xn[...], w1[:, n:n + 512])).astype(BF)
            for n in range(0, D, 512):
                z[r, n:n + 512] = (z[r, n:n + 512].astype(F32) + mm(hid[...], w2[:, n:n + 512])).astype(BF)
            return c
        lax.fori_loop(0, tokens // TILE, ffn_tile, 0)
        prefetch(layer, 5)
        prefetch(layer, 6)
        return carry
    lax.fori_loop(0, 2, layer_step, 0)
    out_copy = pltpu.make_async_copy(z, out_hbm, sem_y)
    out_copy.start()
    out_copy.wait()


def decode(lens, y, h1, h2, wqkv, wo, wq, wkv, woc, w1, w2):
    n_seq = lens.shape[0]
    tokens = n_seq * S_DEC
    pad = n_seq // 2 * S_ENC + S_ENC
    cost = pl.CostEstimate(flops=150_000_000_000, bytes_accessed=100_000_000, transcendentals=0)
    return pl.pallas_call(
        lambda *refs: dec_kernel(n_seq, *refs),
        out_shape=jax.ShapeDtypeStruct((tokens, D), BF),
        in_specs=[SMEM] + [ANY] * 10,
        out_specs=ANY,
        scratch_shapes=[
            pltpu.SMEM((n_seq,), jnp.int32),
            pltpu.VMEM((tokens, D), BF),
            pltpu.VMEM((pad, 2 * D), BF),
            pltpu.VMEM((2, TILE, D), BF),
            pltpu.VMEM((DTILE, 6 * D), BF),
            pltpu.VMEM((DTILE, 2 * D), BF),
            pltpu.VMEM((32, 2 * S_DEC, S_ENC), F32),
            pltpu.VMEM((32, 2 * S_DEC, S_ENC), BF),
            pltpu.VMEM((TILE, D), BF),
            pltpu.VMEM((TILE, FF), BF),
            pltpu.VMEM((D, 6 * D), BF),
            pltpu.VMEM((2 * D, D), BF),
            pltpu.VMEM((D, 2 * D), BF),
            pltpu.VMEM((D, 2 * D), BF),
            pltpu.VMEM((2 * D, D), BF),
            pltpu.VMEM((D, FF), BF),
            pltpu.VMEM((FF, D), BF),
            pltpu.SemaphoreType.DMA,
            pltpu.SemaphoreType.DMA((84,)),
            pltpu.SemaphoreType.DMA((2,)),
        ],
        compiler_params=pltpu.CompilerParams(vmem_limit_bytes=VMEM_LIMIT),
        cost_estimate=cost,
        name="decode",
    )(lens, y, h1, h2, wqkv, wo, wq, wkv, woc, w1, w2)


def by_head(w):
    return w.reshape(w.shape[0], D, -1, HD).transpose(0, 2, 1, 3)


def solution(mesh):
    stages = mesh.shape["stage"]
    swap = [(source, (source + stages // 2) % stages) for source in range(stages)]
    rows = P(("data", "stage"))
    whole = P()

    def body(x_enc, enc_len, y, enc_wqkv, enc_wo, enc_w1, enc_w2, dec_wqkv, dec_wo, cross_wq, cross_wkv, cross_wo, dec_w1, dec_w2):
        n_seq = x_enc.shape[0]
        n_half = n_seq // 2
        layers = enc_wqkv.shape[0]
        x_recv = lax.ppermute(x_enc[n_half:].reshape(n_half * S_ENC, D), "stage", swap)
        len_recv = lax.ppermute(enc_len, "stage", swap)
        e_w = (by_head(enc_wqkv), enc_wo.reshape(layers, 2 * D, D), enc_w1, enc_w2)
        h_own = encode(enc_len[:n_half], x_enc.reshape(n_seq * S_ENC, D), *e_w)
        h_first = lax.ppermute(h_own, "stage", swap)
        h_second = encode(len_recv[n_half:], x_recv, *e_w)
        out = decode(
            len_recv, y.reshape(n_seq * S_DEC, D), h_first, h_second,
            by_head(dec_wqkv), dec_wo.reshape(layers, 2 * D, D),
            by_head(cross_wq), by_head(cross_wkv), cross_wo.reshape(layers, 2 * D, D),
            dec_w1, dec_w2)
        return out.reshape(n_seq, S_DEC, D)

    return jax.shard_map(body, mesh=mesh, in_specs=(rows, rows, rows) + (whole,) * 11, out_specs=rows, check_vma=False)
```

```python
import jax
import jax.numpy as jnp
from jax import lax
from jax.experimental import pallas as pl
from jax.experimental.pallas import tpu as pltpu
from jax.sharding import PartitionSpec as P

BF = jnp.bfloat16
F32 = jnp.float32
D = 1024
HEADS = 16
HD = 128
FF = 3072
S_ENC = 128
S_DEC = 48
TILE = 256
DTILE = 192
GROUP = 4
SEQS = 3
SLOTS = 4
CHUNK = 64
LOG2E = 1.4426950408889634
SCALE2 = HD ** -0.5 * LOG2E
VMEM_LIMIT = 67_000_000


def rms(h):
    wide = h.astype(F32)
    return (wide * lax.rsqrt(jnp.mean(wide * wide, axis=-1, keepdims=True) + 1e-6)).astype(BF)


def mm(lhs, rhs):
    return jnp.dot(lhs, rhs, preferred_element_type=F32)


def gelu(v):
    return jax.nn.gelu(v, approximate=True)


def softmax(s):
    m = jnp.max(s, axis=-1, keepdims=True)
    e = jnp.exp2((s - m) * SCALE2)
    return (e * (1.0 / jnp.sum(e, axis=-1, keepdims=True))).astype(BF)


def qk(q, k):
    return lax.dot_general(q, k, (((1,), (1,)), ((), ())), preferred_element_type=F32)


def prefix_starts(len_ref, starts, n):
    def step(i, pos):
        starts[i] = pos
        return pos + ((len_ref[i] + 15) // 16) * 16
    return lax.fori_loop(0, n, step, jnp.int32(0))


def head_copies(hbm, buf, sem, layer, heads, first):
    return [pltpu.make_async_copy(hbm.at[layer, c], buf.at[:, c * HD:(c + 1) * HD], sem.at[first + c]) for c in heads]


def start_all(copies):
    for c in copies:
        c.start()


def wait_all(copies):
    for c in copies:
        c.wait()


def relay(n, copy, body):
    for j in range(SLOTS):
        copy(j, j).start()

    def step(j, c):
        slot = lax.rem(j, SLOTS)
        copy(j, slot).wait()
        body(j, slot)

        @pl.when(j + SLOTS < n)
        def _():
            copy(j + SLOTS, slot).start()
        return c
    lax.fori_loop(0, n, step, 0)


def relay_heads(hbm, layer, raw, sem, buf, n_t, heads):
    blocks = D // CHUNK

    def rows_of(j):
        return pl.ds(pl.multiple_of(lax.rem(j, blocks) * CHUNK, CHUNK), CHUNK)

    def copy(j, slot):
        j = jnp.int32(j)
        return pltpu.make_async_copy(hbm.at[layer, rows_of(j), lax.div(j, blocks)], raw.at[slot], sem.at[slot])

    def body(j, slot):
        y = jnp.swapaxes(raw[slot], 0, 1)
        t = lax.div(j, blocks)
        for c in range(heads):
            buf[rows_of(j), pl.ds(pl.multiple_of((t * heads + c) * HD, HD), HD)] = y[c]
    relay(blocks * n_t, copy, body)


def enc_kernel(n_seq, fresh, len_ref, x_hbm, wqkv_hbm, wo_hbm, w1_hbm, w2_hbm, out_hbm, *rest):
    flat_hbm = None
    if fresh:
        flat_hbm, *rest = rest
    starts, h, qkv_a, qkv_b, o, s_scr, p_scr, xn, hid, wqkv, wo, w1, w2, raw, sem_x, sem_w, sem_r, sem_o = rest
    gw = GROUP * HD
    n_step = (n_seq + SEQS - 1) // SEQS

    def qkv_copy(layer):
        if fresh:
            return pltpu.make_async_copy(wqkv, flat_hbm.at[layer], sem_w.at[0])
        return pltpu.make_async_copy(wqkv_hbm.at[layer], wqkv, sem_w.at[0])

    def late_copies(layer):
        return [pltpu.make_async_copy(src.at[layer], dst, sem_w.at[k])
                for k, (src, dst) in enumerate(((wo_hbm, wo), (w1_hbm, w1), (w2_hbm, w2)), 1)]

    total = prefix_starts(len_ref, starts, n_seq)
    nt = (total + TILE - 1) // TILE
    end = pl.multiple_of(nt * TILE, TILE)
    last = pl.multiple_of((nt - 1) * TILE, TILE)
    h[pl.ds(last, TILE), :] = jnp.zeros((TILE, D), BF)

    def x_copy(s, j):
        src = x_hbm.at[pl.ds(pl.multiple_of(s * S_ENC + j * 16, 16), 16), :]
        dst = h.at[pl.ds(pl.multiple_of(starts[s] + j * 16, 16), 16), :]
        return pltpu.make_async_copy(src, dst, sem_x)

    def each_piece(fn):
        def seq(s, c):
            lax.fori_loop(0, (len_ref[s] + 15) // 16, lambda j, d: (fn(s, j), d)[1], 0)
            return c
        lax.fori_loop(0, n_seq, seq, 0)

    each_piece(lambda s, j: x_copy(s, j).start())
    if not fresh:
        qkv_copy(0).start()
    o[pl.ds(last, TILE), :] = jnp.zeros((TILE, HEADS * HD), BF)
    for buf in (qkv_a, qkv_b):
        buf[pl.ds(end, S_ENC), :] = jnp.zeros((S_ENC, 3 * gw), BF)
    each_piece(lambda s, j: x_copy(s, j).wait())

    def layer_step(layer, carry):
        if fresh:
            relay_heads(wqkv_hbm, layer, raw, sem_r, wqkv, 3, HEADS)
        else:
            qkv_copy(layer).wait()

        @pl.when(layer == 0)
        def _():
            start_all(late_copies(0))

        def project_part(i, g, t, dst):
            r = pl.ds(pl.multiple_of(i * TILE, TILE), TILE)
            c0 = pl.ds(pl.multiple_of((t * HEADS + g * GROUP) * HD, gw), gw)
            dst[r, t * gw:(t + 1) * gw] = mm(xn[...], wqkv[:, c0]).astype(BF)

        def norm(i):
            xn[...] = rms(h[pl.ds(pl.multiple_of(i * TILE, TILE), TILE), :])

        def seq_of(i, b):
            s = jnp.minimum(SEQS * i + b, n_seq - 1)
            return s, pl.ds(pl.multiple_of(starts[s], 16), S_ENC)

        def scores(i, buf):
            for b in range(SEQS):
                s, r = seq_of(i, b)
                keep = lax.broadcasted_iota(jnp.int32, (S_ENC, S_ENC), 1) < len_ref[s]
                for hh in range(GROUP):
                    c = hh * HD
                    s_scr[b * GROUP + hh] = jnp.where(keep, qk(buf[r, c:c + HD], buf[r, gw + c:gw + c + HD]), -1e30)

        def probs():
            for j in range(SEQS * GROUP):
                p_scr[j] = softmax(s_scr[j])

        def values(i, g, buf):
            for b in range(SEQS):
                s, r = seq_of(i, b)
                for hh in range(GROUP):
                    c = hh * HD
                    oc = pl.ds(pl.multiple_of(g * gw + c, HD), HD)
                    o[r, oc] = mm(p_scr[b * GROUP + hh], buf[r, 2 * gw + c:2 * gw + c + HD]).astype(BF)

        def project_only(i, c):
            norm(i)
            for t in range(3):
                project_part(i, 0, t, qkv_a)
            return c
        lax.fori_loop(0, nt, project_only, 0)
        if fresh:
            qkv_copy(layer).start()

        def attend(g, src, dst, n_both):
            def both(i, c):
                scores(i, src)
                norm(i)
                project_part(i, g + 1, 0, dst)
                probs()
                project_part(i, g + 1, 1, dst)
                project_part(i, g + 1, 2, dst)
                values(i, g, src)
                return c

            def attend_only(i, c):
                scores(i, src)
                probs()
                values(i, g, src)
                return c
            lax.fori_loop(0, n_both, both, 0)
            lax.fori_loop(n_both, n_step, attend_only, 0)

        def two_groups(gp, c):
            attend(2 * gp, qkv_a, qkv_b, nt)
            attend(2 * gp + 1, qkv_b, qkv_a, jnp.where(gp == HEADS // GROUP // 2 - 1, 0, nt))
            return c
        lax.fori_loop(0, HEADS // GROUP // 2, two_groups, 0)

        if fresh:
            qkv_copy(layer).wait()
        else:
            @pl.when(layer == 0)
            def _():
                qkv_copy(1).start()

        wait_all(late_copies(layer))

        def ffn_tile(i, c):
            r = pl.ds(pl.multiple_of(i * TILE, TILE), TILE)
            for n in range(0, D, 512):
                h[r, n:n + 512] = (h[r, n:n + 512].astype(F32) + mm(o[r, :], wo[:, n:n + 512])).astype(BF)
            xn[...] = rms(h[r, :])
            for n in range(0, FF, 512):
                hid[:, n:n + 512] = gelu(mm(xn[...], w1[:, n:n + 512])).astype(BF)
            for n in range(0, D, 512):
                h[r, n:n + 512] = (h[r, n:n + 512].astype(F32) + mm(hid[...], w2[:, n:n + 512])).astype(BF)
            return c
        lax.fori_loop(0, nt, ffn_tile, 0)

        @pl.when(layer == 0)
        def _():
            start_all(late_copies(1))
        return carry
    lax.fori_loop(0, 2, layer_step, 0)

    def out_copy(i):
        r = pl.ds(pl.multiple_of(i * TILE, TILE), TILE)
        return pltpu.make_async_copy(h.at[r, :], out_hbm.at[r, :], sem_o)

    def out_tile(i, c):
        r = pl.ds(pl.multiple_of(i * TILE, TILE), TILE)
        h[r, :] = rms(h[r, :])

        @pl.when(i > 0)
        def _():
            out_copy(i - 1).start()
        return c
    lax.fori_loop(0, nt, out_tile, 0)
    out_copy(nt - 1).start()
    lax.fori_loop(0, nt, lambda i, c: (out_copy(i).wait(), c)[1], 0)


ANY = pl.BlockSpec(memory_space=pl.ANY)
SMEM = pl.BlockSpec(memory_space=pltpu.SMEM)


def encode(fresh, lens, x, wqkv, wo, w1, w2):
    n_seq = lens.shape[0]
    rows = n_seq * S_ENC
    pad = rows + S_ENC
    tokens = rows * 5 // 8
    cost = pl.CostEstimate(flops=tokens * 2 * 30_400_000, bytes_accessed=70_000_000, transcendentals=0)
    out_shape = [jax.ShapeDtypeStruct((rows, D), BF)]
    if fresh:
        out_shape.append(jax.ShapeDtypeStruct((wqkv.shape[0], D, 6 * D), BF))
    return pl.pallas_call(
        lambda *refs: enc_kernel(n_seq, fresh, *refs),
        out_shape=out_shape,
        in_specs=[SMEM] + [ANY] * 5,
        out_specs=[ANY] * len(out_shape),
        scratch_shapes=[
            pltpu.SMEM((n_seq,), jnp.int32),
            pltpu.VMEM((rows, D), BF),
            pltpu.VMEM((pad, 3 * GROUP * HD), BF),
            pltpu.VMEM((pad, 3 * GROUP * HD), BF),
            pltpu.VMEM((pad, 2 * D), BF),
            pltpu.VMEM((SEQS * GROUP, S_ENC, S_ENC), F32),
            pltpu.VMEM((SEQS * GROUP, S_ENC, S_ENC), BF),
            pltpu.VMEM((TILE, D), BF),
            pltpu.VMEM((TILE, FF), BF),
            pltpu.VMEM((D, 6 * D), BF),
            pltpu.VMEM((2 * D, D), BF),
            pltpu.VMEM((D, FF), BF),
            pltpu.VMEM((FF, D), BF),
            pltpu.VMEM((SLOTS, CHUNK, HEADS, HD), BF),
            pltpu.SemaphoreType.DMA,
            pltpu.SemaphoreType.DMA((4,)),
            pltpu.SemaphoreType.DMA((SLOTS,)),
            pltpu.SemaphoreType.DMA,
        ],
        compiler_params=pltpu.CompilerParams(vmem_limit_bytes=VMEM_LIMIT),
        cost_estimate=cost,
        name="encode_first" if fresh else "encode_second",
    )(lens, x, wqkv, wo, w1, w2)


def dec_kernel(n_seq, len_ref, y_hbm, h1_hbm, h2_hbm, wqkv_hbm, wo_hbm, wq_hbm, wkv_hbm, woc_hbm, w1_hbm, w2_hbm, out_hbm,
               starts, z, kv, ht, qkv, o, s_scr, p_scr, xn, hid, wqkv, wo, wq, wkv, woc, w1, w2, raw, raw8, sem_y, sem_w, sem_r, sem_h):
    tokens = n_seq * S_DEC
    n_half = n_seq // 2
    def q_copies(layer):
        return head_copies(wq_hbm, wq, sem_w, layer, range(HEADS), 5)

    def w_copy(layer, k):
        src, dst = ((wo_hbm, wo), (woc_hbm, woc), (w1_hbm, w1), (w2_hbm, w2))[k]
        return pltpu.make_async_copy(src.at[layer], dst, sem_w.at[k])

    y_copy = pltpu.make_async_copy(y_hbm, z, sem_y)
    y_copy.start()

    def step(i, pos):
        pos = jnp.where(i == n_half, 0, pos)
        starts[i] = pos
        return pos + ((len_ref[i] + 15) // 16) * 16

    def total_of(lo):
        return lax.fori_loop(lo, lo + n_half, lambda i, t: t + ((len_ref[i] + 15) // 16) * 16, jnp.int32(0))
    lax.fori_loop(0, n_seq, step, jnp.int32(0))
    y_copy.wait()

    pair = 2 * S_DEC
    qpos = lax.broadcasted_iota(jnp.int32, (pair, pair), 0)
    kpos = lax.broadcasted_iota(jnp.int32, (pair, pair), 1)
    causal = (kpos <= qpos) & ((kpos >= S_DEC) == (qpos >= S_DEC))

    def prefetch(layer, copies):
        @pl.when(layer == 0)
        def _():
            start_all(copies)

    def layer_step(layer, carry):
        relay_heads(wqkv_hbm, layer, raw, sem_r, wqkv, 3, HEADS)
        prefetch(layer, [w_copy(0, k) for k in range(4)] + q_copies(0))
        w_copy(layer, 0).wait()

        def self_tile(i, c):
            r = pl.ds(pl.multiple_of(i * DTILE, DTILE), DTILE)
            xn[:DTILE, :] = rms(z[r, :])
            gw = GROUP * HD
            n_groups = HEADS // GROUP
            n_pairs = DTILE // pair

            def project(g):
                for t in range(3):
                    c0 = t * 2 * D + g * gw
                    qkv[:, c0:c0 + gw] = mm(xn[:DTILE, :], wqkv[:, c0:c0 + gw]).astype(BF)

            def scores(g):
                for b in range(n_pairs):
                    rr = slice(b * pair, (b + 1) * pair)
                    for hh in range(GROUP):
                        c0 = g * gw + hh * HD
                        sc = qk(qkv[rr, c0:c0 + HD], qkv[rr, 2 * D + c0:2 * D + c0 + HD])
                        s_scr[(g % 2) * 16 + b * GROUP + hh, :, :pair] = jnp.where(causal, sc, -1e30)

            def values(g):
                for b in range(n_pairs):
                    rr = slice(b * pair, (b + 1) * pair)
                    for hh in range(GROUP):
                        c0 = g * gw + hh * HD
                        p = p_scr[(g % 2) * 16 + b * GROUP + hh, :, :pair]
                        o[rr, c0:c0 + HD] = mm(p, qkv[rr, 4 * D + c0:4 * D + c0 + HD]).astype(BF)

            def probs(g):
                for j in range(n_pairs * GROUP):
                    j = (g % 2) * 16 + j
                    p_scr[j, :, :pair] = softmax(s_scr[j, :, :pair])

            for g in range(n_groups + 1):
                if g < n_groups:
                    project(g)
                    scores(g)
                    probs(g)
                if g > 0:
                    values(g - 1)
            for n in range(0, D, 512):
                z[r, n:n + 512] = (z[r, n:n + 512].astype(F32) + mm(o[...], wo[:, n:n + 512])).astype(BF)
            return c
        lax.fori_loop(0, tokens // DTILE, self_tile, 0)
        prefetch(layer, [w_copy(1, 0)])
        relay_heads(wkv_hbm, layer, raw8, sem_r, wkv, 2, HEADS // 2)
        wait_all(q_copies(layer))
        w_copy(layer, 1).wait()

        def half_step(hf, carry):
            nt = (total_of(hf * n_half) + TILE - 1) // TILE

            def h_copy(i, src_hbm=h1_hbm):
                src = src_hbm.at[pl.ds(pl.multiple_of(i * TILE, TILE), TILE), :]
                return pltpu.make_async_copy(src, ht.at[lax.rem(i, 2)], sem_h.at[lax.rem(i, 2)])

            def h_start(i):
                @pl.when(hf == 0)
                def _():
                    h_copy(i, h1_hbm).start()

                @pl.when(hf == 1)
                def _():
                    h_copy(i, h2_hbm).start()
            h_start(jnp.int32(0))
            kv[pl.ds(pl.multiple_of(nt * TILE, TILE), S_ENC), :] = jnp.zeros((S_ENC, 2 * D), BF)

            def kv_tile(i, c):
                @pl.when(i + 1 < nt)
                def _():
                    h_start(i + 1)
                h_copy(i).wait()
                r = pl.ds(pl.multiple_of(i * TILE, TILE), TILE)
                for n in range(0, 2 * D, D):
                    kv[r, n:n + D] = mm(ht[lax.rem(i, 2)], wkv[:, n:n + D]).astype(BF)
                return c
            lax.fori_loop(0, nt, kv_tile, 0)

            def cross_tile(i, c):
                base = hf * n_half
                r = pl.ds(pl.multiple_of(base * S_DEC + i * DTILE, DTILE), DTILE)
                xn[:DTILE, :] = rms(z[r, :])
                n_b = DTILE // S_DEC
                gw = 2 * GROUP * HD

                def project(g):
                    qkv[:, g * gw:(g + 1) * gw] = mm(xn[:DTILE, :], wq[:, g * gw:(g + 1) * gw]).astype(BF)

                def where_of(b):
                    s = base + i * n_b + b
                    return s, pl.ds(pl.multiple_of(starts[s], 16), S_ENC), slice(b * S_DEC, (b + 1) * S_DEC)

                def scores(g):
                    for b in range(n_b):
                        s, kr, rr = where_of(b)
                        keep = lax.broadcasted_iota(jnp.int32, (pair, S_ENC), 1) < len_ref[s]
                        for hh in range(GROUP):
                            c0 = g * gw + 2 * hh * HD
                            k0 = (g * GROUP + hh) * HD
                            q2 = jnp.concatenate([qkv[rr, c0:c0 + HD], qkv[rr, c0 + HD:c0 + 2 * HD]], axis=0)
                            s_scr[g * 16 + b * GROUP + hh] = jnp.where(keep, qk(q2, kv[kr, k0:k0 + HD]), -1e30)

                def probs(g):
                    for j in range(16):
                        p_scr[g * 16 + j] = softmax(s_scr[g * 16 + j])

                def values(g):
                    for b in range(n_b):
                        s, kr, rr = where_of(b)
                        for hh in range(GROUP):
                            c0 = g * gw + 2 * hh * HD
                            k0 = D + (g * GROUP + hh) * HD
                            res = mm(p_scr[g * 16 + b * GROUP + hh], kv[kr, k0:k0 + HD]).astype(BF)
                            o[rr, c0:c0 + HD] = res[:S_DEC]
                            o[rr, c0 + HD:c0 + 2 * HD] = res[S_DEC:]

                project(0)
                scores(0)
                probs(0)
                project(1)
                scores(1)
                probs(1)
                values(0)
                values(1)
                for n in range(0, D, 512):
                    z[r, n:n + 512] = (z[r, n:n + 512].astype(F32) + mm(o[...], woc[:, n:n + 512])).astype(BF)
                return c
            lax.fori_loop(0, n_half * S_DEC // DTILE, cross_tile, 0)
            return carry
        lax.fori_loop(0, 2, half_step, 0)
        prefetch(layer, q_copies(1) + [w_copy(1, 1)])

        w_copy(layer, 2).wait()
        w_copy(layer, 3).wait()

        def ffn_tile(i, c):
            r = pl.ds(pl.multiple_of(i * TILE, TILE), TILE)
            xn[...] = rms(z[r, :])
            for n in range(0, FF, 512):
                hid[:, n:n + 512] = gelu(mm(xn[...], w1[:, n:n + 512])).astype(BF)
            for n in range(0, D, 512):
                z[r, n:n + 512] = (z[r, n:n + 512].astype(F32) + mm(hid[...], w2[:, n:n + 512])).astype(BF)
            return c
        lax.fori_loop(0, tokens // TILE, ffn_tile, 0)
        prefetch(layer, [w_copy(1, 2), w_copy(1, 3)])
        return carry
    lax.fori_loop(0, 2, layer_step, 0)
    out_copy = pltpu.make_async_copy(z, out_hbm, sem_y)
    out_copy.start()
    out_copy.wait()


def decode(lens, y, h1, h2, wqkv, wo, wq, wkv, woc, w1, w2):
    n_seq = lens.shape[0]
    tokens = n_seq * S_DEC
    pad = n_seq // 2 * S_ENC + S_ENC
    cost = pl.CostEstimate(flops=150_000_000_000, bytes_accessed=100_000_000, transcendentals=0)
    return pl.pallas_call(
        lambda *refs: dec_kernel(n_seq, *refs),
        out_shape=jax.ShapeDtypeStruct((tokens, D), BF),
        in_specs=[SMEM] + [ANY] * 10,
        out_specs=ANY,
        scratch_shapes=[
            pltpu.SMEM((n_seq,), jnp.int32),
            pltpu.VMEM((tokens, D), BF),
            pltpu.VMEM((pad, 2 * D), BF),
            pltpu.VMEM((2, TILE, D), BF),
            pltpu.VMEM((DTILE, 6 * D), BF),
            pltpu.VMEM((DTILE, 2 * D), BF),
            pltpu.VMEM((32, 2 * S_DEC, S_ENC), F32),
            pltpu.VMEM((32, 2 * S_DEC, S_ENC), BF),
            pltpu.VMEM((TILE, D), BF),
            pltpu.VMEM((TILE, FF), BF),
            pltpu.VMEM((D, 6 * D), BF),
            pltpu.VMEM((2 * D, D), BF),
            pltpu.VMEM((D, 2 * D), BF),
            pltpu.VMEM((D, 2 * D), BF),
            pltpu.VMEM((2 * D, D), BF),
            pltpu.VMEM((D, FF), BF),
            pltpu.VMEM((FF, D), BF),
            pltpu.VMEM((SLOTS, CHUNK, HEADS, HD), BF),
            pltpu.VMEM((SLOTS, CHUNK, HEADS // 2, HD), BF),
            pltpu.SemaphoreType.DMA,
            pltpu.SemaphoreType.DMA((21,)),
            pltpu.SemaphoreType.DMA((SLOTS,)),
            pltpu.SemaphoreType.DMA((2,)),
        ],
        compiler_params=pltpu.CompilerParams(vmem_limit_bytes=VMEM_LIMIT),
        cost_estimate=cost,
        name="decode",
    )(lens, y, h1, h2, wqkv, wo, wq, wkv, woc, w1, w2)


def by_head(w):
    return w.reshape(w.shape[0], D, -1, HD).transpose(0, 2, 1, 3)


def solution(mesh):
    stages = mesh.shape["stage"]
    swap = [(source, (source + stages // 2) % stages) for source in range(stages)]
    rows = P(("data", "stage"))
    whole = P()

    def body(x_enc, enc_len, y, enc_wqkv, enc_wo, enc_w1, enc_w2, dec_wqkv, dec_wo, cross_wq, cross_wkv, cross_wo, dec_w1, dec_w2):
        n_seq = x_enc.shape[0]
        n_half = n_seq // 2
        layers = enc_wqkv.shape[0]
        x_recv = lax.ppermute(x_enc[n_half:].reshape(n_half * S_ENC, D), "stage", swap)
        len_recv = lax.ppermute(enc_len, "stage", swap)
        e_w = (enc_wo.reshape(layers, 2 * D, D), enc_w1, enc_w2)
        h_own, wqkv_flat = encode(True, enc_len[:n_half], x_enc.reshape(n_seq * S_ENC, D), enc_wqkv, *e_w)
        h_first = lax.ppermute(h_own, "stage", swap)
        h_second, = encode(False, len_recv[n_half:], x_recv, wqkv_flat, *e_w)
        out = decode(
            len_recv, y.reshape(n_seq * S_DEC, D), h_first, h_second,
            dec_wqkv, dec_wo.reshape(layers, 2 * D, D),
            by_head(cross_wq), cross_wkv, cross_wo.reshape(layers, 2 * D, D),
            dec_w1, dec_w2)
        return out.reshape(n_seq, S_DEC, D)

    return jax.shard_map(body, mesh=mesh, in_specs=(rows, rows, rows) + (whole,) * 11, out_specs=rows, check_vma=False)
```

```python
import jax
import jax.numpy as jnp
from jax import lax
from jax.experimental import pallas as pl
from jax.experimental.pallas import tpu as pltpu
from jax.sharding import PartitionSpec as P

BF = jnp.bfloat16
F32 = jnp.float32
D = 1024
HEADS = 16
HD = 128
FF = 3072
S_ENC = 128
S_DEC = 48
TILE = 256
DTILE = 192
GROUP = 4
SEQS = 3
SLOTS = 12
CHUNK = 64
LOG2E = 1.4426950408889634
SCALE2 = HD ** -0.5 * LOG2E
VMEM_LIMIT = 67_000_000


def rms(h):
    wide = h.astype(F32)
    return (wide * lax.rsqrt(jnp.mean(wide * wide, axis=-1, keepdims=True) + 1e-6)).astype(BF)


def mm(lhs, rhs):
    return jnp.dot(lhs, rhs, preferred_element_type=F32)


def gelu(v):
    return jax.nn.gelu(v, approximate=True)


def softmax(s):
    m = jnp.max(s, axis=-1, keepdims=True)
    e = jnp.exp2((s - m) * SCALE2)
    return (e * (1.0 / jnp.sum(e, axis=-1, keepdims=True))).astype(BF)


def qk(q, k):
    return lax.dot_general(q, k, (((1,), (1,)), ((), ())), preferred_element_type=F32)


def prefix_starts(len_ref, starts, n):
    def step(i, pos):
        starts[i] = pos
        return pos + ((len_ref[i] + 15) // 16) * 16
    return lax.fori_loop(0, n, step, jnp.int32(0))


def head_copies(hbm, buf, sem, layer, heads, first):
    return [pltpu.make_async_copy(hbm.at[layer, c], buf.at[:, c * HD:(c + 1) * HD], sem.at[first + c]) for c in heads]


def start_all(copies):
    for c in copies:
        c.start()


def wait_all(copies):
    for c in copies:
        c.wait()


class Relay:
    def __init__(self, hbm, raw, sem, buf):
        self.hbm, self.raw, self.sem, self.buf = hbm, raw, sem, buf
        self.slots = raw.shape[0]
        self.blocks = D // CHUNK
        self.n = self.blocks * hbm.shape[2]

    def rows_of(self, j):
        return pl.ds(pl.multiple_of(lax.rem(j, self.blocks) * CHUNK, CHUNK), CHUNK)

    def copy(self, layer, j):
        slot = lax.rem(j, self.slots)
        return pltpu.make_async_copy(
            self.hbm.at[layer, self.rows_of(j), lax.div(j, self.blocks)], self.raw.at[slot], self.sem.at[slot])

    def start(self, layer):
        for j in range(min(self.slots, self.n)):
            self.copy(layer, jnp.int32(j)).start()

    def run(self, layer):
        def step(j, c):
            self.copy(layer, j).wait()
            y = jnp.swapaxes(self.raw[lax.rem(j, self.slots)], 0, 1)
            t = lax.div(j, self.blocks)
            for h in range(HEADS):
                self.buf[self.rows_of(j), pl.ds(pl.multiple_of((t * HEADS + h) * HD, HD), HD)] = y[h]

            @pl.when(j + self.slots < self.n)
            def _():
                self.copy(layer, j + self.slots).start()
            return c
        lax.fori_loop(0, self.n, step, 0)


def enc_kernel(n_seq, fresh, len_ref, x_hbm, wqkv_hbm, wo_hbm, w1_hbm, w2_hbm, out_hbm, *rest):
    flat_hbm = None
    if fresh:
        flat_hbm, *rest = rest
    starts, h, qkv_a, qkv_b, o, s_scr, p_scr, xn, hid, wqkv, wo, w1, w2, raw, sem_x, sem_w, sem_r, sem_o = rest
    gw = GROUP * HD
    n_step = (n_seq + SEQS - 1) // SEQS

    def flat_copy(layer):
        return pltpu.make_async_copy(wqkv, flat_hbm.at[layer], sem_w.at[0])

    def group_copies(layer, g):
        copies = []
        for t in range(3):
            cols = pl.ds(pl.multiple_of((t * HEADS + g * GROUP) * HD, gw), gw)
            copies.append(pltpu.make_async_copy(wqkv_hbm.at[layer, :, cols], wqkv.at[:, cols], sem_w.at[4 + 3 * g + t]))
        return copies

    relay = Relay(wqkv_hbm, raw, sem_r, wqkv) if fresh else None

    def late_copies(layer):
        return [pltpu.make_async_copy(src.at[layer], dst, sem_w.at[k])
                for k, (src, dst) in enumerate(((wo_hbm, wo), (w1_hbm, w1), (w2_hbm, w2)), 1)]

    total = prefix_starts(len_ref, starts, n_seq)
    nt = (total + TILE - 1) // TILE
    end = pl.multiple_of(nt * TILE, TILE)
    last = pl.multiple_of((nt - 1) * TILE, TILE)
    h[pl.ds(last, TILE), :] = jnp.zeros((TILE, D), BF)

    def x_copy(s, j):
        src = x_hbm.at[pl.ds(pl.multiple_of(s * S_ENC + j * 16, 16), 16), :]
        dst = h.at[pl.ds(pl.multiple_of(starts[s] + j * 16, 16), 16), :]
        return pltpu.make_async_copy(src, dst, sem_x)

    def each_piece(fn):
        def seq(s, c):
            lax.fori_loop(0, (len_ref[s] + 15) // 16, lambda j, d: (fn(s, j), d)[1], 0)
            return c
        lax.fori_loop(0, n_seq, seq, 0)

    each_piece(lambda s, j: x_copy(s, j).start())
    if fresh:
        relay.start(0)
    else:
        for g in range(HEADS // GROUP):
            start_all(group_copies(0, g))
    o[pl.ds(last, TILE), :] = jnp.zeros((TILE, HEADS * HD), BF)
    for buf in (qkv_a, qkv_b):
        buf[pl.ds(end, S_ENC), :] = jnp.zeros((S_ENC, 3 * gw), BF)
    each_piece(lambda s, j: x_copy(s, j).wait())

    def layer_step(layer, carry):
        if fresh:
            relay.run(layer)
        else:
            wait_all(group_copies(layer, 0))

        @pl.when(layer == 0)
        def _():
            start_all(late_copies(0))

        def project_part(i, g, t, dst):
            r = pl.ds(pl.multiple_of(i * TILE, TILE), TILE)
            c0 = pl.ds(pl.multiple_of((t * HEADS + g * GROUP) * HD, gw), gw)
            dst[r, t * gw:(t + 1) * gw] = mm(xn[...], wqkv[:, c0]).astype(BF)

        def norm(i):
            xn[...] = rms(h[pl.ds(pl.multiple_of(i * TILE, TILE), TILE), :])

        def seq_of(i, b):
            s = jnp.minimum(SEQS * i + b, n_seq - 1)
            return s, pl.ds(pl.multiple_of(starts[s], 16), S_ENC)

        def scores(i, buf):
            for b in range(SEQS):
                s, r = seq_of(i, b)
                keep = lax.broadcasted_iota(jnp.int32, (S_ENC, S_ENC), 1) < len_ref[s]
                for hh in range(GROUP):
                    c = hh * HD
                    s_scr[b * GROUP + hh] = jnp.where(keep, qk(buf[r, c:c + HD], buf[r, gw + c:gw + c + HD]), -1e30)

        def probs():
            for j in range(SEQS * GROUP):
                p_scr[j] = softmax(s_scr[j])

        def values(i, g, buf):
            for b in range(SEQS):
                s, r = seq_of(i, b)
                for hh in range(GROUP):
                    c = hh * HD
                    oc = pl.ds(pl.multiple_of(g * gw + c, HD), HD)
                    o[r, oc] = mm(p_scr[b * GROUP + hh], buf[r, 2 * gw + c:2 * gw + c + HD]).astype(BF)

        def project_only(i, c):
            norm(i)
            for t in range(3):
                project_part(i, 0, t, qkv_a)
            return c
        lax.fori_loop(0, nt, project_only, 0)
        if fresh:
            flat_copy(layer).start()

        def attend(g, src, dst, n_both):
            def both(i, c):
                scores(i, src)
                norm(i)
                project_part(i, g + 1, 0, dst)
                probs()
                project_part(i, g + 1, 1, dst)
                project_part(i, g + 1, 2, dst)
                values(i, g, src)
                return c

            def attend_only(i, c):
                scores(i, src)
                probs()
                values(i, g, src)
                return c
            lax.fori_loop(0, n_both, both, 0)
            lax.fori_loop(n_both, n_step, attend_only, 0)

        def two_groups(gp, c):
            more = gp < HEADS // GROUP // 2 - 1
            if not fresh:
                wait_all(group_copies(layer, 2 * gp + 1))
            attend(2 * gp, qkv_a, qkv_b, nt)
            if not fresh:
                @pl.when(more)
                def _():
                    wait_all(group_copies(layer, 2 * gp + 2))
            attend(2 * gp + 1, qkv_b, qkv_a, jnp.where(more, nt, 0))
            return c
        lax.fori_loop(0, HEADS // GROUP // 2, two_groups, 0)

        if fresh:
            flat_copy(layer).wait()

        @pl.when(layer == 0)
        def _():
            if fresh:
                relay.start(1)
            else:
                for g in range(HEADS // GROUP):
                    start_all(group_copies(1, g))

        wait_all(late_copies(layer))

        def ffn_tile(i, c):
            r = pl.ds(pl.multiple_of(i * TILE, TILE), TILE)
            for n in range(0, D, 512):
                h[r, n:n + 512] = (h[r, n:n + 512].astype(F32) + mm(o[r, :], wo[:, n:n + 512])).astype(BF)
            xn[...] = rms(h[r, :])
            for n in range(0, FF, 512):
                hid[:, n:n + 512] = gelu(mm(xn[...], w1[:, n:n + 512])).astype(BF)
            for n in range(0, D, 512):
                h[r, n:n + 512] = (h[r, n:n + 512].astype(F32) + mm(hid[...], w2[:, n:n + 512])).astype(BF)
            return c
        lax.fori_loop(0, nt, ffn_tile, 0)

        @pl.when(layer == 0)
        def _():
            start_all(late_copies(1))
        return carry
    lax.fori_loop(0, 2, layer_step, 0)

    def out_copy(i):
        r = pl.ds(pl.multiple_of(i * TILE, TILE), TILE)
        return pltpu.make_async_copy(h.at[r, :], out_hbm.at[r, :], sem_o)

    def out_tile(i, c):
        r = pl.ds(pl.multiple_of(i * TILE, TILE), TILE)
        h[r, :] = rms(h[r, :])

        @pl.when(i > 0)
        def _():
            out_copy(i - 1).start()
        return c
    lax.fori_loop(0, nt, out_tile, 0)
    out_copy(nt - 1).start()
    lax.fori_loop(0, nt, lambda i, c: (out_copy(i).wait(), c)[1], 0)


ANY = pl.BlockSpec(memory_space=pl.ANY)
SMEM = pl.BlockSpec(memory_space=pltpu.SMEM)


def encode(fresh, lens, x, wqkv, wo, w1, w2):
    n_seq = lens.shape[0]
    rows = n_seq * S_ENC
    pad = rows + S_ENC
    tokens = rows * 5 // 8
    cost = pl.CostEstimate(flops=tokens * 2 * 30_400_000, bytes_accessed=70_000_000, transcendentals=0)
    out_shape = [jax.ShapeDtypeStruct((rows, D), BF)]
    if fresh:
        out_shape.append(jax.ShapeDtypeStruct((wqkv.shape[0], D, 6 * D), BF))
    return pl.pallas_call(
        lambda *refs: enc_kernel(n_seq, fresh, *refs),
        out_shape=out_shape,
        in_specs=[SMEM] + [ANY] * 5,
        out_specs=[ANY] * len(out_shape),
        scratch_shapes=[
            pltpu.SMEM((n_seq,), jnp.int32),
            pltpu.VMEM((rows, D), BF),
            pltpu.VMEM((pad, 3 * GROUP * HD), BF),
            pltpu.VMEM((pad, 3 * GROUP * HD), BF),
            pltpu.VMEM((pad, 2 * D), BF),
            pltpu.VMEM((SEQS * GROUP, S_ENC, S_ENC), F32),
            pltpu.VMEM((SEQS * GROUP, S_ENC, S_ENC), BF),
            pltpu.VMEM((TILE, D), BF),
            pltpu.VMEM((TILE, FF), BF),
            pltpu.VMEM((D, 6 * D), BF),
            pltpu.VMEM((2 * D, D), BF),
            pltpu.VMEM((D, FF), BF),
            pltpu.VMEM((FF, D), BF),
            pltpu.VMEM((16, CHUNK, HEADS, HD), BF),
            pltpu.SemaphoreType.DMA,
            pltpu.SemaphoreType.DMA((16,)),
            pltpu.SemaphoreType.DMA((16,)),
            pltpu.SemaphoreType.DMA,
        ],
        compiler_params=pltpu.CompilerParams(vmem_limit_bytes=VMEM_LIMIT),
        cost_estimate=cost,
        name="encode_first" if fresh else "encode_second",
    )(lens, x, wqkv, wo, w1, w2)


def dec_kernel(n_seq, len_ref, y_hbm, h1_hbm, h2_hbm, wqkv_hbm, wo_hbm, wq_hbm, wkv_hbm, woc_hbm, w1_hbm, w2_hbm, out_hbm,
               starts, z, kv, ht, wide, o, s_scr, p_scr, xn, wqkv, wo, wq, wkv, woc, w1, w2, raw, sem_y, sem_w, sem_r, sem_h):
    tokens = n_seq * S_DEC
    n_half = n_seq // 2
    qkv = wide.at[:DTILE]
    hid = wide.at[:, :FF]
    relay_qkv = Relay(wqkv_hbm, raw, sem_r, wqkv)
    relay_kv = Relay(wkv_hbm, raw, sem_r, wkv)
    relay_qkv.start(0)

    def q_copies(layer):
        return head_copies(wq_hbm, wq, sem_w, layer, range(HEADS), 5)

    def w_copy(layer, k):
        src, dst = ((wo_hbm, wo), (woc_hbm, woc), (w1_hbm, w1), (w2_hbm, w2))[k]
        return pltpu.make_async_copy(src.at[layer], dst, sem_w.at[k])

    y_copy = pltpu.make_async_copy(y_hbm, z, sem_y)
    y_copy.start()

    def step(i, pos):
        pos = jnp.where(i == n_half, 0, pos)
        starts[i] = pos
        return pos + ((len_ref[i] + 15) // 16) * 16

    def total_of(lo):
        return lax.fori_loop(lo, lo + n_half, lambda i, t: t + ((len_ref[i] + 15) // 16) * 16, jnp.int32(0))
    lax.fori_loop(0, n_seq, step, jnp.int32(0))
    y_copy.wait()

    pair = 2 * S_DEC
    qpos = lax.broadcasted_iota(jnp.int32, (pair, pair), 0)
    kpos = lax.broadcasted_iota(jnp.int32, (pair, pair), 1)
    causal = (kpos <= qpos) & ((kpos >= S_DEC) == (qpos >= S_DEC))

    def prefetch(layer, copies):
        @pl.when(layer == 0)
        def _():
            start_all(copies)

    def layer_step(layer, carry):
        relay_qkv.run(layer)
        relay_kv.start(layer)
        prefetch(layer, [w_copy(0, k) for k in range(4)] + q_copies(0))
        w_copy(layer, 0).wait()

        def self_tile(i, c):
            r = pl.ds(pl.multiple_of(i * DTILE, DTILE), DTILE)
            xn[:DTILE, :] = rms(z[r, :])
            gw = GROUP * HD
            n_groups = HEADS // GROUP
            n_pairs = DTILE // pair

            def project(g):
                for t in range(3):
                    c0 = t * 2 * D + g * gw
                    qkv[:, c0:c0 + gw] = mm(xn[:DTILE, :], wqkv[:, c0:c0 + gw]).astype(BF)

            def scores(g):
                for b in range(n_pairs):
                    rr = slice(b * pair, (b + 1) * pair)
                    for hh in range(GROUP):
                        c0 = g * gw + hh * HD
                        sc = qk(qkv[rr, c0:c0 + HD], qkv[rr, 2 * D + c0:2 * D + c0 + HD])
                        s_scr[(g % 2) * 16 + b * GROUP + hh, :, :pair] = jnp.where(causal, sc, -1e30)

            def values(g):
                for b in range(n_pairs):
                    rr = slice(b * pair, (b + 1) * pair)
                    for hh in range(GROUP):
                        c0 = g * gw + hh * HD
                        p = p_scr[(g % 2) * 16 + b * GROUP + hh, :, :pair]
                        o[rr, c0:c0 + HD] = mm(p, qkv[rr, 4 * D + c0:4 * D + c0 + HD]).astype(BF)

            def probs(g):
                for j in range(n_pairs * GROUP):
                    j = (g % 2) * 16 + j
                    p_scr[j, :, :pair] = softmax(s_scr[j, :, :pair])

            for g in range(n_groups + 1):
                if g < n_groups:
                    project(g)
                    scores(g)
                    probs(g)
                if g > 0:
                    values(g - 1)
            for n in range(0, D, 512):
                z[r, n:n + 512] = (z[r, n:n + 512].astype(F32) + mm(o[...], wo[:, n:n + 512])).astype(BF)
            return c
        lax.fori_loop(0, tokens // DTILE, self_tile, 0)
        prefetch(layer, [w_copy(1, 0)])
        relay_kv.run(layer)
        wait_all(q_copies(layer))
        w_copy(layer, 1).wait()

        def half_step(hf, carry):
            nt = (total_of(hf * n_half) + TILE - 1) // TILE

            def h_copy(i, src_hbm=h1_hbm):
                src = src_hbm.at[pl.ds(pl.multiple_of(i * TILE, TILE), TILE), :]
                return pltpu.make_async_copy(src, ht.at[lax.rem(i, 2)], sem_h.at[lax.rem(i, 2)])

            def h_start(i):
                @pl.when(hf == 0)
                def _():
                    h_copy(i, h1_hbm).start()

                @pl.when(hf == 1)
                def _():
                    h_copy(i, h2_hbm).start()
            h_start(jnp.int32(0))
            kv[pl.ds(pl.multiple_of(nt * TILE, TILE), S_ENC), :] = jnp.zeros((S_ENC, 2 * D), BF)

            def kv_tile(i, c):
                @pl.when(i + 1 < nt)
                def _():
                    h_start(i + 1)
                h_copy(i).wait()
                r = pl.ds(pl.multiple_of(i * TILE, TILE), TILE)
                for n in range(0, 2 * D, D):
                    kv[r, n:n + D] = mm(ht[lax.rem(i, 2)], wkv[:, n:n + D]).astype(BF)
                return c
            lax.fori_loop(0, nt, kv_tile, 0)

            def cross_tile(i, c):
                base = hf * n_half
                r = pl.ds(pl.multiple_of(base * S_DEC + i * DTILE, DTILE), DTILE)
                xn[:DTILE, :] = rms(z[r, :])
                n_b = DTILE // S_DEC
                gw = 2 * GROUP * HD

                def project(g):
                    qkv[:, g * gw:(g + 1) * gw] = mm(xn[:DTILE, :], wq[:, g * gw:(g + 1) * gw]).astype(BF)

                def where_of(b):
                    s = base + i * n_b + b
                    return s, pl.ds(pl.multiple_of(starts[s], 16), S_ENC), slice(b * S_DEC, (b + 1) * S_DEC)

                def scores(g):
                    for b in range(n_b):
                        s, kr, rr = where_of(b)
                        keep = lax.broadcasted_iota(jnp.int32, (pair, S_ENC), 1) < len_ref[s]
                        for hh in range(GROUP):
                            c0 = g * gw + 2 * hh * HD
                            k0 = (g * GROUP + hh) * HD
                            q2 = jnp.concatenate([qkv[rr, c0:c0 + HD], qkv[rr, c0 + HD:c0 + 2 * HD]], axis=0)
                            s_scr[g * 16 + b * GROUP + hh] = jnp.where(keep, qk(q2, kv[kr, k0:k0 + HD]), -1e30)

                def probs(g):
                    for j in range(16):
                        p_scr[g * 16 + j] = softmax(s_scr[g * 16 + j])

                def values(g):
                    for b in range(n_b):
                        s, kr, rr = where_of(b)
                        for hh in range(GROUP):
                            c0 = g * gw + 2 * hh * HD
                            k0 = D + (g * GROUP + hh) * HD
                            res = mm(p_scr[g * 16 + b * GROUP + hh], kv[kr, k0:k0 + HD]).astype(BF)
                            o[rr, c0:c0 + HD] = res[:S_DEC]
                            o[rr, c0 + HD:c0 + 2 * HD] = res[S_DEC:]

                project(0)
                scores(0)
                probs(0)
                project(1)
                scores(1)
                probs(1)
                values(0)
                values(1)
                for n in range(0, D, 512):
                    z[r, n:n + 512] = (z[r, n:n + 512].astype(F32) + mm(o[...], woc[:, n:n + 512])).astype(BF)
                return c
            lax.fori_loop(0, n_half * S_DEC // DTILE, cross_tile, 0)
            return carry
        lax.fori_loop(0, 2, half_step, 0)
        prefetch(layer, q_copies(1) + [w_copy(1, 1)])

        @pl.when(layer == 0)
        def _():
            relay_qkv.start(1)

        w_copy(layer, 2).wait()
        w_copy(layer, 3).wait()

        def ffn_tile(i, c):
            r = pl.ds(pl.multiple_of(i * TILE, TILE), TILE)
            xn[...] = rms(z[r, :])
            for n in range(0, FF, 512):
                hid[:, n:n + 512] = gelu(mm(xn[...], w1[:, n:n + 512])).astype(BF)
            for n in range(0, D, 512):
                z[r, n:n + 512] = (z[r, n:n + 512].astype(F32) + mm(hid[...], w2[:, n:n + 512])).astype(BF)
            return c
        lax.fori_loop(0, tokens // TILE, ffn_tile, 0)
        prefetch(layer, [w_copy(1, 2), w_copy(1, 3)])
        return carry
    lax.fori_loop(0, 2, layer_step, 0)
    out_copy = pltpu.make_async_copy(z, out_hbm, sem_y)
    out_copy.start()
    out_copy.wait()


def decode(lens, y, h1, h2, wqkv, wo, wq, wkv, woc, w1, w2):
    n_seq = lens.shape[0]
    tokens = n_seq * S_DEC
    pad = n_seq // 2 * S_ENC + S_ENC
    cost = pl.CostEstimate(flops=150_000_000_000, bytes_accessed=100_000_000, transcendentals=0)
    return pl.pallas_call(
        lambda *refs: dec_kernel(n_seq, *refs),
        out_shape=jax.ShapeDtypeStruct((tokens, D), BF),
        in_specs=[SMEM] + [ANY] * 10,
        out_specs=ANY,
        scratch_shapes=[
            pltpu.SMEM((n_seq,), jnp.int32),
            pltpu.VMEM((tokens, D), BF),
            pltpu.VMEM((pad, 2 * D), BF),
            pltpu.VMEM((2, TILE, D), BF),
            pltpu.VMEM((TILE, 6 * D), BF),
            pltpu.VMEM((DTILE, 2 * D), BF),
            pltpu.VMEM((32, 2 * S_DEC, S_ENC), F32),
            pltpu.VMEM((32, 2 * S_DEC, S_ENC), BF),
            pltpu.VMEM((TILE, D), BF),
            pltpu.VMEM((D, 6 * D), BF),
            pltpu.VMEM((2 * D, D), BF),
            pltpu.VMEM((D, 2 * D), BF),
            pltpu.VMEM((D, 2 * D), BF),
            pltpu.VMEM((2 * D, D), BF),
            pltpu.VMEM((D, FF), BF),
            pltpu.VMEM((FF, D), BF),
            pltpu.VMEM((SLOTS, CHUNK, HEADS, HD), BF),
            pltpu.SemaphoreType.DMA,
            pltpu.SemaphoreType.DMA((21,)),
            pltpu.SemaphoreType.DMA((SLOTS,)),
            pltpu.SemaphoreType.DMA((2,)),
        ],
        compiler_params=pltpu.CompilerParams(vmem_limit_bytes=VMEM_LIMIT),
        cost_estimate=cost,
        name="decode",
    )(lens, y, h1, h2, wqkv, wo, wq, wkv, woc, w1, w2)


def by_head(w):
    return w.reshape(w.shape[0], D, -1, HD).transpose(0, 2, 1, 3)


def solution(mesh):
    stages = mesh.shape["stage"]
    swap = [(source, (source + stages // 2) % stages) for source in range(stages)]
    rows = P(("data", "stage"))
    whole = P()

    def body(x_enc, enc_len, y, enc_wqkv, enc_wo, enc_w1, enc_w2, dec_wqkv, dec_wo, cross_wq, cross_wkv, cross_wo, dec_w1, dec_w2):
        n_seq = x_enc.shape[0]
        n_half = n_seq // 2
        layers = enc_wqkv.shape[0]
        x_recv = lax.ppermute(x_enc[n_half:].reshape(n_half * S_ENC, D), "stage", swap)
        len_recv = lax.ppermute(enc_len, "stage", swap)
        e_w = (enc_wo.reshape(layers, 2 * D, D), enc_w1, enc_w2)
        h_own, wqkv_flat = encode(True, enc_len[:n_half], x_enc.reshape(n_seq * S_ENC, D), enc_wqkv, *e_w)
        h_first = lax.ppermute(h_own, "stage", swap)
        h_second, = encode(False, len_recv[n_half:], x_recv, wqkv_flat, *e_w)
        out = decode(
            len_recv, y.reshape(n_seq * S_DEC, D), h_first, h_second,
            dec_wqkv, dec_wo.reshape(layers, 2 * D, D),
            by_head(cross_wq), cross_wkv.reshape(layers, D, 1, HEADS, HD), cross_wo.reshape(layers, 2 * D, D),
            dec_w1, dec_w2)
        return out.reshape(n_seq, S_DEC, D)

    return jax.shard_map(body, mesh=mesh, in_specs=(rows, rows, rows) + (whole,) * 11, out_specs=rows, check_vma=False)
```

```python
import jax
import jax.numpy as jnp
from jax import lax
from jax.experimental import pallas as pl
from jax.experimental.pallas import tpu as pltpu
from jax.sharding import PartitionSpec as P

BF = jnp.bfloat16
F32 = jnp.float32
D = 1024
HEADS = 16
HD = 128
FF = 3072
S_ENC = 128
S_DEC = 48
TILE = 256
DTILE = 192
GROUP = 4
SEQS = 3
SLOTS = 12
CHUNK = 64
LOG2E = 1.4426950408889634
SCALE2 = HD ** -0.5 * LOG2E
VMEM_LIMIT = 67_000_000


def rms(h):
    wide = h.astype(F32)
    return (wide * lax.rsqrt(jnp.mean(wide * wide, axis=-1, keepdims=True) + 1e-6)).astype(BF)


def mm(lhs, rhs):
    return jnp.dot(lhs, rhs, preferred_element_type=F32)


def gelu(v):
    return jax.nn.gelu(v, approximate=True)


def softmax(s):
    m = jnp.max(s, axis=-1, keepdims=True)
    e = jnp.exp2((s - m) * SCALE2)
    return (e * (1.0 / jnp.sum(e, axis=-1, keepdims=True))).astype(BF)


def qk(q, k):
    return lax.dot_general(q, k, (((1,), (1,)), ((), ())), preferred_element_type=F32)


def prefix_starts(len_ref, starts, n):
    def step(i, pos):
        starts[i] = pos
        return pos + ((len_ref[i] + 15) // 16) * 16
    return lax.fori_loop(0, n, step, jnp.int32(0))


def head_copies(hbm, buf, sem, layer, heads, first):
    return [pltpu.make_async_copy(hbm.at[layer, c], buf.at[:, c * HD:(c + 1) * HD], sem.at[first + c]) for c in heads]


def start_all(copies):
    for c in copies:
        c.start()


def wait_all(copies):
    for c in copies:
        c.wait()


class Relay:
    def __init__(self, hbm, raw, sem, buf):
        self.hbm, self.raw, self.sem, self.buf = hbm, raw, sem, buf
        self.slots = raw.shape[0]
        self.blocks = D // CHUNK
        self.n = self.blocks * hbm.shape[2]

    def rows_of(self, j):
        return pl.ds(pl.multiple_of(lax.rem(j, self.blocks) * CHUNK, CHUNK), CHUNK)

    def copy(self, layer, j):
        slot = lax.rem(j, self.slots)
        return pltpu.make_async_copy(
            self.hbm.at[layer, self.rows_of(j), lax.div(j, self.blocks)], self.raw.at[slot], self.sem.at[slot])

    def start(self, layer):
        for j in range(min(self.slots, self.n)):
            self.copy(layer, jnp.int32(j)).start()

    def run(self, layer):
        def step(j, c):
            self.copy(layer, j).wait()
            y = jnp.swapaxes(self.raw[lax.rem(j, self.slots)], 0, 1)
            t = lax.div(j, self.blocks)
            for h in range(HEADS):
                self.buf[self.rows_of(j), pl.ds(pl.multiple_of((t * HEADS + h) * HD, HD), HD)] = y[h]

            @pl.when(j + self.slots < self.n)
            def _():
                self.copy(layer, j + self.slots).start()
            return c
        lax.fori_loop(0, self.n, step, 0)


def enc_kernel(n_seq, fresh, len_ref, x_hbm, wqkv_hbm, wo_hbm, w1_hbm, w2_hbm, out_hbm, *rest):
    flat_hbm = None
    if fresh:
        flat_hbm, *rest = rest
    starts, h, qkv_a, qkv_b, o, s_scr, p_scr, xn, hid, wqkv, wo, w1, w2, raw, sem_x, sem_w, sem_r, sem_o = rest
    gw = GROUP * HD
    n_step = (n_seq + SEQS - 1) // SEQS

    def flat_copy(layer):
        return pltpu.make_async_copy(wqkv, flat_hbm.at[layer], sem_w.at[0])

    def group_copies(layer, g):
        copies = []
        for t in range(3):
            cols = pl.ds(pl.multiple_of((t * HEADS + g * GROUP) * HD, gw), gw)
            copies.append(pltpu.make_async_copy(wqkv_hbm.at[layer, :, cols], wqkv.at[:, cols], sem_w.at[4 + 3 * g + t]))
        return copies

    relay = Relay(wqkv_hbm, raw, sem_r, wqkv) if fresh else None

    def late_copies(layer):
        return [pltpu.make_async_copy(src.at[layer], dst, sem_w.at[k])
                for k, (src, dst) in enumerate(((wo_hbm, wo), (w1_hbm, w1), (w2_hbm, w2)), 1)]

    total = prefix_starts(len_ref, starts, n_seq)
    nt = (total + TILE - 1) // TILE
    end = pl.multiple_of(nt * TILE, TILE)
    last = pl.multiple_of((nt - 1) * TILE, TILE)
    h[pl.ds(last, TILE), :] = jnp.zeros((TILE, D), BF)

    def x_copy(s, j):
        src = x_hbm.at[pl.ds(pl.multiple_of(s * S_ENC + j * 16, 16), 16), :]
        dst = h.at[pl.ds(pl.multiple_of(starts[s] + j * 16, 16), 16), :]
        return pltpu.make_async_copy(src, dst, sem_x)

    def each_piece(fn):
        def seq(s, c):
            lax.fori_loop(0, (len_ref[s] + 15) // 16, lambda j, d: (fn(s, j), d)[1], 0)
            return c
        lax.fori_loop(0, n_seq, seq, 0)

    each_piece(lambda s, j: x_copy(s, j).start())
    if fresh:
        relay.start(0)
    else:
        for g in range(HEADS // GROUP):
            start_all(group_copies(0, g))
    o[pl.ds(last, TILE), :] = jnp.zeros((TILE, HEADS * HD), BF)
    for buf in (qkv_a, qkv_b):
        buf[pl.ds(end, S_ENC), :] = jnp.zeros((S_ENC, 3 * gw), BF)
    each_piece(lambda s, j: x_copy(s, j).wait())

    def layer_step(layer, carry):
        if fresh:
            relay.run(layer)
        else:
            wait_all(group_copies(layer, 0))

        @pl.when(layer == 0)
        def _():
            start_all(late_copies(0))

        def project_part(i, g, t, dst):
            r = pl.ds(pl.multiple_of(i * TILE, TILE), TILE)
            c0 = pl.ds(pl.multiple_of((t * HEADS + g * GROUP) * HD, gw), gw)
            dst[r, t * gw:(t + 1) * gw] = mm(xn[...], wqkv[:, c0]).astype(BF)

        def norm(i):
            xn[...] = rms(h[pl.ds(pl.multiple_of(i * TILE, TILE), TILE), :])

        def seq_of(i, b):
            s = jnp.minimum(SEQS * i + b, n_seq - 1)
            return s, pl.ds(pl.multiple_of(starts[s], 16), S_ENC)

        def scores(i, buf):
            for b in range(SEQS):
                s, r = seq_of(i, b)
                keep = lax.broadcasted_iota(jnp.int32, (S_ENC, S_ENC), 1) < len_ref[s]
                for hh in range(GROUP):
                    c = hh * HD
                    s_scr[b * GROUP + hh] = jnp.where(keep, qk(buf[r, c:c + HD], buf[r, gw + c:gw + c + HD]), -1e30)

        def probs():
            for j in range(SEQS * GROUP):
                p_scr[j] = softmax(s_scr[j])

        def values(i, g, buf):
            for b in range(SEQS):
                s, r = seq_of(i, b)
                for hh in range(GROUP):
                    c = hh * HD
                    oc = pl.ds(pl.multiple_of(g * gw + c, HD), HD)
                    o[r, oc] = mm(p_scr[b * GROUP + hh], buf[r, 2 * gw + c:2 * gw + c + HD]).astype(BF)

        def project_only(i, c):
            norm(i)
            for t in range(3):
                project_part(i, 0, t, qkv_a)
            return c
        lax.fori_loop(0, nt, project_only, 0)
        if fresh:
            flat_copy(layer).start()

        def attend(g, src, dst, n_both):
            def both(i, c):
                scores(i, src)
                norm(i)
                project_part(i, g + 1, 0, dst)
                probs()
                project_part(i, g + 1, 1, dst)
                project_part(i, g + 1, 2, dst)
                values(i, g, src)
                return c

            def attend_only(i, c):
                scores(i, src)
                probs()
                values(i, g, src)
                return c
            lax.fori_loop(0, n_both, both, 0)
            lax.fori_loop(n_both, n_step, attend_only, 0)

        def two_groups(gp, c):
            more = gp < HEADS // GROUP // 2 - 1
            if not fresh:
                wait_all(group_copies(layer, 2 * gp + 1))
            attend(2 * gp, qkv_a, qkv_b, nt)
            if not fresh:
                @pl.when(more)
                def _():
                    wait_all(group_copies(layer, 2 * gp + 2))
            attend(2 * gp + 1, qkv_b, qkv_a, jnp.where(more, nt, 0))
            return c
        lax.fori_loop(0, HEADS // GROUP // 2, two_groups, 0)

        if fresh:
            flat_copy(layer).wait()

        @pl.when(layer == 0)
        def _():
            if fresh:
                relay.start(1)
            else:
                for g in range(HEADS // GROUP):
                    start_all(group_copies(1, g))

        wait_all(late_copies(layer))

        def ffn_tile(i, c):
            r = pl.ds(pl.multiple_of(i * TILE, TILE), TILE)
            for n in range(0, D, 512):
                h[r, n:n + 512] = (h[r, n:n + 512].astype(F32) + mm(o[r, :], wo[:, n:n + 512])).astype(BF)
            xn[...] = rms(h[r, :])
            for n in range(0, FF, 512):
                hid[:, n:n + 512] = gelu(mm(xn[...], w1[:, n:n + 512])).astype(BF)
            for n in range(0, D, 512):
                h[r, n:n + 512] = (h[r, n:n + 512].astype(F32) + mm(hid[...], w2[:, n:n + 512])).astype(BF)
            return c
        lax.fori_loop(0, nt, ffn_tile, 0)

        @pl.when(layer == 0)
        def _():
            start_all(late_copies(1))
        return carry
    lax.fori_loop(0, 2, layer_step, 0)

    def out_copy(i):
        r = pl.ds(pl.multiple_of(i * TILE, TILE), TILE)
        return pltpu.make_async_copy(h.at[r, :], out_hbm.at[r, :], sem_o)

    def out_tile(i, c):
        r = pl.ds(pl.multiple_of(i * TILE, TILE), TILE)
        h[r, :] = rms(h[r, :])

        @pl.when(i > 0)
        def _():
            out_copy(i - 1).start()
        return c
    lax.fori_loop(0, nt, out_tile, 0)
    out_copy(nt - 1).start()
    lax.fori_loop(0, nt, lambda i, c: (out_copy(i).wait(), c)[1], 0)


ANY = pl.BlockSpec(memory_space=pl.ANY)
SMEM = pl.BlockSpec(memory_space=pltpu.SMEM)


def encode(fresh, lens, x, wqkv, wo, w1, w2):
    n_seq = lens.shape[0]
    rows = n_seq * S_ENC
    pad = rows + S_ENC
    tokens = rows * 5 // 8
    cost = pl.CostEstimate(flops=tokens * 2 * 30_400_000, bytes_accessed=70_000_000, transcendentals=0)
    out_shape = [jax.ShapeDtypeStruct((rows, D), BF)]
    if fresh:
        out_shape.append(jax.ShapeDtypeStruct((wqkv.shape[0], D, 6 * D), BF))
    return pl.pallas_call(
        lambda *refs: enc_kernel(n_seq, fresh, *refs),
        out_shape=out_shape,
        in_specs=[SMEM] + [ANY] * 5,
        out_specs=[ANY] * len(out_shape),
        scratch_shapes=[
            pltpu.SMEM((n_seq,), jnp.int32),
            pltpu.VMEM((rows, D), BF),
            pltpu.VMEM((pad, 3 * GROUP * HD), BF),
            pltpu.VMEM((pad, 3 * GROUP * HD), BF),
            pltpu.VMEM((pad, 2 * D), BF),
            pltpu.VMEM((SEQS * GROUP, S_ENC, S_ENC), F32),
            pltpu.VMEM((SEQS * GROUP, S_ENC, S_ENC), BF),
            pltpu.VMEM((TILE, D), BF),
            pltpu.VMEM((TILE, FF), BF),
            pltpu.VMEM((D, 6 * D), BF),
            pltpu.VMEM((2 * D, D), BF),
            pltpu.VMEM((D, FF), BF),
            pltpu.VMEM((FF, D), BF),
            pltpu.VMEM((16, CHUNK, HEADS, HD), BF),
            pltpu.SemaphoreType.DMA,
            pltpu.SemaphoreType.DMA((16,)),
            pltpu.SemaphoreType.DMA((16,)),
            pltpu.SemaphoreType.DMA,
        ],
        compiler_params=pltpu.CompilerParams(vmem_limit_bytes=VMEM_LIMIT),
        cost_estimate=cost,
        name="encode_first" if fresh else "encode_second",
    )(lens, x, wqkv, wo, w1, w2)


def dec_kernel(n_seq, len_ref, y_hbm, h1_hbm, h2_hbm, wqkv_hbm, wo_hbm, wq_hbm, wkv_hbm, woc_hbm, w1_hbm, w2_hbm, out_hbm,
               starts, z, kv, ht, qkv, o, s_scr, p_scr, xn, hid, wqkv, wo, wq, wkv, woc, w1, w2, raw, sem_y, sem_w, sem_r, sem_h):
    tokens = n_seq * S_DEC
    n_half = n_seq // 2
    relay_qkv = Relay(wqkv_hbm, raw, sem_r, wqkv)
    relay_kv = Relay(wkv_hbm, raw, sem_r, wkv)
    relay_qkv.start(0)

    def q_copies(layer):
        return head_copies(wq_hbm, wq, sem_w, layer, range(HEADS), 5)

    def w_copy(layer, k):
        src, dst = ((wo_hbm, wo), (woc_hbm, woc), (w1_hbm, w1), (w2_hbm, w2))[k]
        return pltpu.make_async_copy(src.at[layer], dst, sem_w.at[k])

    y_copy = pltpu.make_async_copy(y_hbm, z, sem_y)
    y_copy.start()

    def step(i, pos):
        pos = jnp.where(i == n_half, 0, pos)
        starts[i] = pos
        return pos + ((len_ref[i] + 15) // 16) * 16

    def total_of(lo):
        return lax.fori_loop(lo, lo + n_half, lambda i, t: t + ((len_ref[i] + 15) // 16) * 16, jnp.int32(0))
    lax.fori_loop(0, n_seq, step, jnp.int32(0))
    y_copy.wait()

    pair = 2 * S_DEC
    qpos = lax.broadcasted_iota(jnp.int32, (pair, pair), 0)
    kpos = lax.broadcasted_iota(jnp.int32, (pair, pair), 1)
    causal = (kpos <= qpos) & ((kpos >= S_DEC) == (qpos >= S_DEC))

    def prefetch(layer, copies):
        @pl.when(layer == 0)
        def _():
            start_all(copies)

    def layer_step(layer, carry):
        relay_qkv.run(layer)
        relay_kv.start(layer)
        prefetch(layer, [w_copy(0, k) for k in range(4)] + q_copies(0))
        w_copy(layer, 0).wait()

        def self_tile(i, c):
            r = pl.ds(pl.multiple_of(i * DTILE, DTILE), DTILE)
            xn[:DTILE, :] = rms(z[r, :])
            gw = GROUP * HD
            n_groups = HEADS // GROUP
            n_pairs = DTILE // pair

            def project(g):
                for t in range(3):
                    c0 = t * 2 * D + g * gw
                    qkv[:, c0:c0 + gw] = mm(xn[:DTILE, :], wqkv[:, c0:c0 + gw]).astype(BF)

            def scores(g):
                for b in range(n_pairs):
                    rr = slice(b * pair, (b + 1) * pair)
                    for hh in range(GROUP):
                        c0 = g * gw + hh * HD
                        sc = qk(qkv[rr, c0:c0 + HD], qkv[rr, 2 * D + c0:2 * D + c0 + HD])
                        s_scr[(g % 2) * 16 + b * GROUP + hh, :, :pair] = jnp.where(causal, sc, -1e30)

            def values(g):
                for b in range(n_pairs):
                    rr = slice(b * pair, (b + 1) * pair)
                    for hh in range(GROUP):
                        c0 = g * gw + hh * HD
                        p = p_scr[(g % 2) * 16 + b * GROUP + hh, :, :pair]
                        o[rr, c0:c0 + HD] = mm(p, qkv[rr, 4 * D + c0:4 * D + c0 + HD]).astype(BF)

            def probs(g):
                for j in range(n_pairs * GROUP):
                    j = (g % 2) * 16 + j
                    p_scr[j, :, :pair] = softmax(s_scr[j, :, :pair])

            for g in range(n_groups + 1):
                if g < n_groups:
                    project(g)
                    scores(g)
                    probs(g)
                if g > 0:
                    values(g - 1)
            for n in range(0, D, 512):
                z[r, n:n + 512] = (z[r, n:n + 512].astype(F32) + mm(o[...], wo[:, n:n + 512])).astype(BF)
            return c
        lax.fori_loop(0, tokens // DTILE, self_tile, 0)
        prefetch(layer, [w_copy(1, 0)])
        relay_kv.run(layer)
        wait_all(q_copies(layer))
        w_copy(layer, 1).wait()

        def half_step(hf, carry):
            nt = (total_of(hf * n_half) + TILE - 1) // TILE

            def h_copy(i, src_hbm=h1_hbm):
                src = src_hbm.at[pl.ds(pl.multiple_of(i * TILE, TILE), TILE), :]
                return pltpu.make_async_copy(src, ht.at[lax.rem(i, 2)], sem_h.at[lax.rem(i, 2)])

            def h_start(i):
                @pl.when(hf == 0)
                def _():
                    h_copy(i, h1_hbm).start()

                @pl.when(hf == 1)
                def _():
                    h_copy(i, h2_hbm).start()
            h_start(jnp.int32(0))
            kv[pl.ds(pl.multiple_of(nt * TILE, TILE), S_ENC), :] = jnp.zeros((S_ENC, 2 * D), BF)

            def kv_tile(i, c):
                @pl.when(i + 1 < nt)
                def _():
                    h_start(i + 1)
                h_copy(i).wait()
                r = pl.ds(pl.multiple_of(i * TILE, TILE), TILE)
                for n in range(0, 2 * D, D):
                    kv[r, n:n + D] = mm(ht[lax.rem(i, 2)], wkv[:, n:n + D]).astype(BF)
                return c
            lax.fori_loop(0, nt, kv_tile, 0)

            def cross_tile(i, c):
                base = hf * n_half
                r = pl.ds(pl.multiple_of(base * S_DEC + i * DTILE, DTILE), DTILE)
                xn[:DTILE, :] = rms(z[r, :])
                n_b = DTILE // S_DEC
                gw = 2 * GROUP * HD

                def project(g):
                    qkv[:, g * gw:(g + 1) * gw] = mm(xn[:DTILE, :], wq[:, g * gw:(g + 1) * gw]).astype(BF)

                def where_of(b):
                    s = base + i * n_b + b
                    return s, pl.ds(pl.multiple_of(starts[s], 16), S_ENC), slice(b * S_DEC, (b + 1) * S_DEC)

                def scores(g):
                    for b in range(n_b):
                        s, kr, rr = where_of(b)
                        keep = lax.broadcasted_iota(jnp.int32, (pair, S_ENC), 1) < len_ref[s]
                        for hh in range(GROUP):
                            c0 = g * gw + 2 * hh * HD
                            k0 = (g * GROUP + hh) * HD
                            q2 = jnp.concatenate([qkv[rr, c0:c0 + HD], qkv[rr, c0 + HD:c0 + 2 * HD]], axis=0)
                            s_scr[g * 16 + b * GROUP + hh] = jnp.where(keep, qk(q2, kv[kr, k0:k0 + HD]), -1e30)

                def probs(g):
                    for j in range(16):
                        p_scr[g * 16 + j] = softmax(s_scr[g * 16 + j])

                def values(g):
                    for b in range(n_b):
                        s, kr, rr = where_of(b)
                        for hh in range(GROUP):
                            c0 = g * gw + 2 * hh * HD
                            k0 = D + (g * GROUP + hh) * HD
                            res = mm(p_scr[g * 16 + b * GROUP + hh], kv[kr, k0:k0 + HD]).astype(BF)
                            o[rr, c0:c0 + HD] = res[:S_DEC]
                            o[rr, c0 + HD:c0 + 2 * HD] = res[S_DEC:]

                project(0)
                scores(0)
                probs(0)
                project(1)
                scores(1)
                probs(1)
                values(0)
                values(1)
                for n in range(0, D, 512):
                    z[r, n:n + 512] = (z[r, n:n + 512].astype(F32) + mm(o[...], woc[:, n:n + 512])).astype(BF)
                return c
            lax.fori_loop(0, n_half * S_DEC // DTILE, cross_tile, 0)
            return carry
        lax.fori_loop(0, 2, half_step, 0)
        prefetch(layer, q_copies(1) + [w_copy(1, 1)])

        @pl.when(layer == 0)
        def _():
            relay_qkv.start(1)

        w_copy(layer, 2).wait()
        w_copy(layer, 3).wait()

        def ffn_tile(i, c):
            r = pl.ds(pl.multiple_of(i * TILE, TILE), TILE)
            xn[...] = rms(z[r, :])
            for n in range(0, FF, 512):
                hid[:, n:n + 512] = gelu(mm(xn[...], w1[:, n:n + 512])).astype(BF)
            for n in range(0, D, 512):
                z[r, n:n + 512] = (z[r, n:n + 512].astype(F32) + mm(hid[...], w2[:, n:n + 512])).astype(BF)
            return c
        lax.fori_loop(0, tokens // TILE, ffn_tile, 0)
        prefetch(layer, [w_copy(1, 2), w_copy(1, 3)])
        return carry
    lax.fori_loop(0, 2, layer_step, 0)
    out_copy = pltpu.make_async_copy(z, out_hbm, sem_y)
    out_copy.start()
    out_copy.wait()


def decode(lens, y, h1, h2, wqkv, wo, wq, wkv, woc, w1, w2):
    n_seq = lens.shape[0]
    tokens = n_seq * S_DEC
    pad = n_seq // 2 * S_ENC + S_ENC
    cost = pl.CostEstimate(flops=150_000_000_000, bytes_accessed=100_000_000, transcendentals=0)
    return pl.pallas_call(
        lambda *refs: dec_kernel(n_seq, *refs),
        out_shape=jax.ShapeDtypeStruct((tokens, D), BF),
        in_specs=[SMEM] + [ANY] * 10,
        out_specs=ANY,
        scratch_shapes=[
            pltpu.SMEM((n_seq,), jnp.int32),
            pltpu.VMEM((tokens, D), BF),
            pltpu.VMEM((pad, 2 * D), BF),
            pltpu.VMEM((2, TILE, D), BF),
            pltpu.VMEM((DTILE, 6 * D), BF),
            pltpu.VMEM((DTILE, 2 * D), BF),
            pltpu.VMEM((32, 2 * S_DEC, S_ENC), F32),
            pltpu.VMEM((32, 2 * S_DEC, S_ENC), BF),
            pltpu.VMEM((TILE, D), BF),
            pltpu.VMEM((TILE, FF), BF),
            pltpu.VMEM((D, 6 * D), BF),
            pltpu.VMEM((2 * D, D), BF),
            pltpu.VMEM((D, 2 * D), BF),
            pltpu.VMEM((D, 2 * D), BF),
            pltpu.VMEM((2 * D, D), BF),
            pltpu.VMEM((D, FF), BF),
            pltpu.VMEM((FF, D), BF),
            pltpu.VMEM((SLOTS, CHUNK, HEADS, HD), BF),
            pltpu.SemaphoreType.DMA,
            pltpu.SemaphoreType.DMA((21,)),
            pltpu.SemaphoreType.DMA((SLOTS,)),
            pltpu.SemaphoreType.DMA((2,)),
        ],
        compiler_params=pltpu.CompilerParams(vmem_limit_bytes=VMEM_LIMIT),
        cost_estimate=cost,
        name="decode",
    )(lens, y, h1, h2, wqkv, wo, wq, wkv, woc, w1, w2)


def by_head(w):
    return w.reshape(w.shape[0], D, -1, HD).transpose(0, 2, 1, 3)


def solution(mesh):
    stages = mesh.shape["stage"]
    swap = [(source, (source + stages // 2) % stages) for source in range(stages)]
    rows = P(("data", "stage"))
    whole = P()

    def body(x_enc, enc_len, y, enc_wqkv, enc_wo, enc_w1, enc_w2, dec_wqkv, dec_wo, cross_wq, cross_wkv, cross_wo, dec_w1, dec_w2):
        n_seq = x_enc.shape[0]
        n_half = n_seq // 2
        layers = enc_wqkv.shape[0]
        x_recv = lax.ppermute(x_enc[n_half:].reshape(n_half * S_ENC, D), "stage", swap)
        len_recv = lax.ppermute(enc_len, "stage", swap)
        e_w = (enc_wo.reshape(layers, 2 * D, D), enc_w1, enc_w2)
        h_own, wqkv_flat = encode(True, enc_len[:n_half], x_enc.reshape(n_seq * S_ENC, D), enc_wqkv, *e_w)
        h_first = lax.ppermute(h_own, "stage", swap)
        h_second, = encode(False, len_recv[n_half:], x_recv, wqkv_flat, *e_w)
        out = decode(
            len_recv, y.reshape(n_seq * S_DEC, D), h_first, h_second,
            dec_wqkv, dec_wo.reshape(layers, 2 * D, D),
            by_head(cross_wq), cross_wkv.reshape(layers, D, 1, HEADS, HD), cross_wo.reshape(layers, 2 * D, D),
            dec_w1, dec_w2)
        return out.reshape(n_seq, S_DEC, D)

    return jax.shard_map(body, mesh=mesh, in_specs=(rows, rows, rows) + (whole,) * 11, out_specs=rows, check_vma=False)
```
